16 devices in a mesh: col: 4 (over z, y), row: 4 (over x, core).
Axes of the slice: x: 2, y: 2, z: 2, core: 2. Of those that a mesh axis runs over, the one named last changes fastest.
Arguments:
- mask: int32 [2048, 65536], P('row', 'col')
- user_emb: bfloat16 [2048, 64], P(('row', 'col'))
- item_emb: bfloat16 [65536, 64], P(('col', 'row'))
- queries: int32 [512], replicated
Outputs:
- output 1: bfloat16 [2048, 64], P(('row', 'col'))
- output 2: bfloat16 [65536, 64], P(('col', 'row'))
- output 3: float32 [512, 65536], P(None, ('col', 'row'))
All inputs are finite; a program needn't handle non-finite values.
Results may differ from the reference program's by a relative error of at most 0.00699888.
Values are sent between devices in bfloat16 or wider.
A program may use at most 1 GiB of HBM per device.

```python
import jax
import jax.numpy as jnp
from jax import lax

USERS = 2048
ITEMS = 65536
EMB = 64
LAYERS = 3
QUERIES = 512


def draw_mask(key):
    k_noise, k_rows, k_cols = jax.random.split(key, 3)
    row_level = jax.random.randint(k_rows, (USERS,), 4, 33)
    col_level = jax.random.randint(k_cols, (ITEMS,), 4, 33)
    noise = jax.random.randint(k_noise, (USERS, ITEMS), 0, 1024)
    return (noise < row_level[:, None] * col_level[None, :]).astype(jnp.int32)


def setup_inputs(seed: int = 0) -> dict:
    key = jax.random.key(seed)
    k_mask, k_user, k_item, k_umean, k_imean, k_query = jax.random.split(key, 6)
    scale = EMB ** -0.25
    user_mean = jax.random.normal(k_umean, (EMB,), jnp.float32)
    item_mean = jax.random.normal(k_imean, (EMB,), jnp.float32)
    user_emb = ((jax.random.normal(k_user, (USERS, EMB), jnp.float32) + user_mean[None, :]) * scale).astype(jnp.bfloat16)
    item_emb = ((jax.random.normal(k_item, (ITEMS, EMB), jnp.float32) + item_mean[None, :]) * scale).astype(jnp.bfloat16)
    queries = jax.random.randint(k_query, (QUERIES,), 0, USERS).astype(jnp.int32)
    return {'mask': draw_mask(k_mask), 'user_emb': user_emb, 'item_emb': item_emb, 'queries': queries}


def norm_adjacency(mask):
    deg_user = jnp.maximum(jnp.sum(mask, axis=1), 1)
    deg_item = jnp.maximum(jnp.sum(mask, axis=0), 1)
    inv_user = lax.rsqrt(deg_user.astype(jnp.float32))
    inv_item = lax.rsqrt(deg_item.astype(jnp.float32))
    return (inv_user[:, None] * mask.astype(jnp.float32) * inv_item[None, :]).astype(jnp.bfloat16)


def reference(mask, user_emb, item_emb, queries):
    norm_adj = norm_adjacency(mask)

    def one_layer(carried, unused):
        user_cur, item_cur, user_sum, item_sum = carried
        user_next = jnp.dot(norm_adj, item_cur, preferred_element_type=jnp.float32).astype(jnp.bfloat16)
        item_next = lax.dot_general(norm_adj, user_cur, (((0,), (0,)), ((), ())), preferred_element_type=jnp.float32).astype(jnp.bfloat16)
        return (user_next, item_next, user_sum + user_next.astype(jnp.float32), item_sum + item_next.astype(jnp.float32)), None

    start_state = (user_emb, item_emb, user_emb.astype(jnp.float32), item_emb.astype(jnp.float32))
    end_state, unused_out = lax.scan(one_layer, start_state, None, length=LAYERS)
    final_user = (end_state[2] / (LAYERS + 1)).astype(jnp.bfloat16)
    final_item = (end_state[3] / (LAYERS + 1)).astype(jnp.bfloat16)
    picked = jnp.take(final_user, queries, axis=0)
    scores = lax.dot_general(picked, final_item, (((1,), (1,)), ((), ())), preferred_element_type=jnp.float32)
    return final_user, final_item, scores
```

```python
import jax
import jax.numpy as jnp
from jax import lax
from jax.experimental import pallas as pl
from jax.experimental.pallas import tpu as pltpu
from jax.sharding import PartitionSpec as P

LAYERS = 3
J = 8
NSLOT = 6
F32, BF16 = jnp.float32, jnp.bfloat16


def nt(a, b):
    return lax.dot_general(a, b, (((1,), (1,)), ((), ())), preferred_element_type=F32)


def nn(a, b):
    return lax.dot_general(a, b, (((1,), (0,)), ((), ())), preferred_element_type=F32)


def remote(src, dst, send, recv, **where):
    return pltpu.make_async_remote_copy(
        src_ref=src, dst_ref=dst, send_sem=send, recv_sem=recv,
        device_id=where, device_id_type=pl.DeviceIdType.MESH)


def make_kernel(users, width, quarter, emb, shard_users, n_query):
    w = quarter // J
    rows_blk = 64
    n_rb = users // rows_blk
    lanes = w // 128

    def kern(mask, item, user, qrow, fu_out, fit_out, qt_out,
             adj, stage, item_vm, panel, ps, pk, rs, rx, isum, ut, u0t, usend, urecv, usum,
             rowacc, invu, di, di_sib, di_chip, di_x, invi, du, acc, fut, futr, fu_full,
             m_sem, i_sem, ps_s, ps_r, tx_s, tx_r, as_s, as_r, ax_s, ax_r, af_s, af_r,
             u_s, u_r, d_s, d_r, dx_s, dx_r, f_s, f_r):
        r = lax.axis_index('row')
        c = lax.axis_index('col')
        sib = r + 1 - 2 * (r % 2)
        xp = (r + 2) % 4
        dg = (sib + 2) % 4
        cols = [(c + k) % 4 for k in (1, 2, 3)]

        def mask_copy(b):
            return pltpu.make_async_copy(
                mask.at[:, pl.ds(pl.multiple_of(b * w, w), w)], stage.at[b % NSLOT], m_sem.at[b % NSLOT])

        for b in range(NSLOT):
            mask_copy(b).start()
        item_copy = pltpu.make_async_copy(item, item_vm, i_sem)
        item_copy.start()

        bar = pltpu.get_barrier_semaphore()
        for q in (sib, xp, dg):
            pl.semaphore_signal(bar, inc=1, device_id={'row': q}, device_id_type=pl.DeviceIdType.MESH)
        for q in cols:
            pl.semaphore_signal(bar, inc=1, device_id={'col': q}, device_id_type=pl.DeviceIdType.MESH)
        pl.semaphore_wait(bar, 6)

        eye = (lax.broadcasted_iota(jnp.int32, (emb, emb), 0)
               == lax.broadcasted_iota(jnp.int32, (emb, emb), 1)).astype(F32).astype(BF16)

        def ps_copy(s, j):
            return remote(ps.at[s, j], rs.at[s, j], ps_s.at[s, j], ps_r.at[s, j], row=sib)

        def tx_copy(s, j):
            return remote(pk.at[s, j, 1], rx.at[s, j], tx_s.at[s, j], tx_r.at[s, j], row=xp)

        def as_copy(s, j, q):
            return remote(panel.at[s, q, j], panel.at[s, q, j], as_s.at[s, j], as_r.at[s, j], row=sib)

        def ax_copy(s, j, q):
            return remote(panel.at[s, q, j], panel.at[s, q, j], ax_s.at[s, j], ax_r.at[s, j], row=xp)

        def af_copy(s, j, q):
            return remote(panel.at[s, q, j], panel.at[s, q, j], af_s.at[s, j], af_r.at[s, j], row=sib)

        def share_item(s, j):
            as_copy(s, j, r).start()
            ax_copy(s, j, r).start()

        item_copy.wait()

        def first_item(j, carry):
            t = nt(eye, item_vm[pl.ds(pl.multiple_of(j * w, w), w), :])
            panel[0, r, j] = t.astype(BF16)
            isum[j] = t
            share_item(0, j)
            return carry

        lax.fori_loop(0, J, first_item, 0)
        u0t[c] = nt(eye, user[...]).astype(BF16)

        def u0_copy(k, src, dst_c):
            return remote(u0t.at[src], u0t.at[src], u_s.at[0, k], u_r.at[0, k], col=dst_c)

        for k in range(3):
            u0_copy(k, c, cols[k]).start()

        rowacc[...] = jnp.zeros_like(rowacc)

        def dis_copy(q):
            return remote(di.at[q], di_sib.at[q], d_s.at[q], d_r.at[q], row=sib)

        def dix_copy(q):
            return remote(di_chip.at[q], di_x.at[q], dx_s.at[q], dx_r.at[q], row=xp)

        def chip_degree(q):
            dis_copy(q).wait_recv()
            di_chip[q] = di[q] + di_sib[q]
            dix_copy(q).start()

        for q in range(4):
            def mask_step(j, carry):
                b = q * J + j
                mask_copy(b).wait()
                slot = b % NSLOT

                def rows_step(rb, csum):
                    rows = pl.ds(pl.multiple_of(rb * rows_blk, rows_blk), rows_blk)
                    m = stage[slot, rows, :].astype(F32)
                    adj[b, rows, :] = m.astype(BF16)
                    part = m[:, :128]
                    for t in range(1, lanes):
                        part = part + m[:, t * 128:(t + 1) * 128]
                    rowacc[rows, :] = rowacc[rows, :] + part
                    for t in range(0, rows_blk, 8):
                        csum = csum + m[t:t + 8, :]
                    return csum

                csum = lax.fori_loop(0, n_rb, rows_step, jnp.zeros((8, w), F32), unroll=2)
                di[q, pl.ds(j, 1), :] = jnp.sum(csum, axis=0, keepdims=True)

                @pl.when(b + NSLOT < 4 * J)
                def _():
                    mask_copy(b + NSLOT).start()
                return carry

            lax.fori_loop(0, J, mask_step, 0)
            dis_copy(q).start()
            if q:
                chip_degree(q - 1)

        du[c] = nt(jnp.ones((8, 128), BF16), rowacc[...].astype(BF16))

        def du_copy(k, src, dst_c):
            return remote(du.at[src], du.at[src], u_s.at[4, k], u_r.at[4, k], col=dst_c)

        for k in range(3):
            du_copy(k, c, cols[k]).start()
        chip_degree(3)
        for k in range(3):
            u0_copy(k, (c + 3 - k) % 4, cols[k]).wait_recv()
        u0 = jnp.concatenate([u0t[k] for k in range(4)], axis=1)
        ut[...] = u0
        usum[...] = u0.astype(F32)
        for k in range(3):
            du_copy(k, (c + 3 - k) % 4, cols[k]).wait_recv()
        deg = ((du[0] + du[1]) + du[2]) + du[3]
        inv_row = lax.rsqrt(jnp.maximum(deg, 1.0))
        invu[...] = jnp.transpose(jnp.broadcast_to(inv_row[0:1, :], (128, users)))
        for q in range(4):
            dix_copy(q).wait_recv()
            invi[q] = lax.rsqrt(jnp.maximum(di_chip[q] + di_x[q], 1.0))

        def form(q, j):
            b = q * J + j

            def rows_step(rb, carry):
                rows = pl.ds(pl.multiple_of(rb * rows_blk, rows_blk), rows_blk)
                m = adj[b, rows, :].astype(F32)
                iu = jnp.concatenate([invu[rows, :]] * lanes, axis=1)
                adj[b, rows, :] = ((iu * m) * invi[q, pl.ds(j, 1), :]).astype(BF16)
                return carry

            lax.fori_loop(0, n_rb, rows_step, 0, unroll=2)

        def sum_send(s, j):
            ps_copy(s, j).wait_recv()
            pk[s, j, 1] = pk[s, j, 1] + rs[s, j, 1]
            tx_copy(s, j).start()

        def item_part(s):
            def step(j, carry):
                if s == 0:
                    for q in (sib, dg, r, xp):
                        form(q, j)
                u = ut[...]
                ps[s, j, 0] = nn(u, adj[sib * J + j])
                ps[s, j, 1] = nn(u, adj[dg * J + j])
                ps_copy(s, j).start()
                pk[s, j, 0] = nn(u, adj[r * J + j])
                pk[s, j, 1] = nn(u, adj[xp * J + j])

                @pl.when(j > 0)
                def _():
                    sum_send(s, j - 1)
                return carry

            lax.fori_loop(0, J, step, 0)
            sum_send(s, J - 1)

        def item_finish(s):
            def step(j, carry):
                tx_copy(s, j).wait_recv()
                v = ((pk[s, j, 0] + rs[s, j, 0]) + rx[s, j]).astype(BF16)
                total = isum[j] + v.astype(F32)
                if s < LAYERS - 1:
                    panel[s + 1, r, j] = v
                    share_item(s + 1, j)
                    isum[j] = total
                else:
                    fit_out[j] = (total / (LAYERS + 1)).astype(BF16)
                return carry

            lax.fori_loop(0, J, step, 0)

        def u_copy(s, k, src, dst_c):
            return remote(usend.at[s], urecv.at[s, src], u_s.at[s + 1, k], u_r.at[s + 1, k], col=dst_c)

        def user_part(s):
            acc[...] = jnp.zeros_like(acc)

            def add(q, j):
                acc[...] = acc[...] + nt(adj[q * J + j], panel[s, q, j])

            def step_own(j, carry):
                as_copy(s, j, sib).wait_recv()
                add(r, j)
                add(sib, j)
                return carry

            def step_far(j, carry):
                ax_copy(s, j, xp).wait_recv()
                af_copy(s, j, xp).start()
                add(xp, j)
                af_copy(s, j, dg).wait_recv()
                add(dg, j)
                return carry

            lax.fori_loop(0, J, step_own, 0)
            lax.fori_loop(0, J, step_far, 0)
            t = jnp.transpose(acc[...])
            usend[s] = t
            urecv[s, c] = t
            for k in range(3):
                u_copy(s, k, c, cols[k]).start()

        def user_finish(s):
            for k in range(3):
                u_copy(s, k, (c + 3 - k) % 4, cols[k]).wait_recv()
            v = (((urecv[s, 0] + urecv[s, 1]) + urecv[s, 2]) + urecv[s, 3]).astype(BF16)
            ut[...] = v
            usum[...] = usum[...] + v.astype(F32)

        item_part(0)
        user_part(0)
        item_finish(0)
        user_finish(0)
        item_part(1)
        user_part(1)
        item_finish(1)
        user_finish(1)
        item_part(2)
        user_part(2)
        user_finish(2)

        fu = usum[...] / (LAYERS + 1)
        fu_full[...] = jnp.transpose(fu)
        fu_out[...] = fu_full[pl.ds(pl.multiple_of(c * shard_users, shard_users), shard_users), :].astype(BF16)
        fut[r] = fu.astype(BF16)

        def fu_copy(k, q, **where):
            return remote(fut.at[q], fut.at[q], f_s.at[k], f_r.at[k], **where)

        fu_copy(0, r, row=sib).start()
        fu_copy(1, r, row=xp).start()
        fu_copy(1, xp, row=xp).wait_recv()
        fu_copy(2, xp, row=sib).start()
        fu_copy(0, sib, row=sib).wait_recv()
        fu_copy(2, dg, row=sib).wait_recv()
        qt = jnp.zeros((emb, n_query), F32)
        for q in range(4):
            ids = lax.broadcasted_iota(jnp.int32, (users, n_query), 0) + q * users
            onehot = jnp.where(ids == qrow[...], 1.0, 0.0).astype(BF16)
            qt = qt + nn(fut[q], onehot)
        qt_out[...] = qt.astype(BF16)

        item_finish(2)

        def drain(j, carry):
            for s in range(3):
                ps_copy(s, j).wait_send()
                tx_copy(s, j).wait_send()
                as_copy(s, j, r).wait_send()
                ax_copy(s, j, r).wait_send()
                af_copy(s, j, xp).wait_send()
            return carry

        lax.fori_loop(0, J, drain, 0)
        for k in range(3):
            u0_copy(k, c, cols[k]).wait_send()
            du_copy(k, c, cols[k]).wait_send()
            for s in range(3):
                u_copy(s, k, c, cols[k]).wait_send()
        for q in range(4):
            dis_copy(q).wait_send()
            dix_copy(q).wait_send()
        fu_copy(0, r, row=sib).wait_send()
        fu_copy(1, r, row=xp).wait_send()
        fu_copy(2, xp, row=sib).wait_send()

    dma = pltpu.SemaphoreType.DMA
    scratch = [
        pltpu.VMEM((4 * J, users, w), BF16),
        pltpu.VMEM((NSLOT, users, w), jnp.int32),
        pltpu.VMEM((quarter, emb), BF16),
        pltpu.VMEM((3, 4, J, emb, w), BF16),
        pltpu.VMEM((3, J, 2, emb, w), F32),
        pltpu.VMEM((3, J, 2, emb, w), F32),
        pltpu.VMEM((3, J, 2, emb, w), F32),
        pltpu.VMEM((3, J, emb, w), F32),
        pltpu.VMEM((J, emb, w), F32),
        pltpu.VMEM((emb, users), BF16),
        pltpu.VMEM((4, emb, shard_users), BF16),
        pltpu.VMEM((3, emb, users), F32),
        pltpu.VMEM((3, 4, emb, users), F32),
        pltpu.VMEM((emb, users), F32),
        pltpu.VMEM((users, 128), F32),
        pltpu.VMEM((users, 128), F32),
        pltpu.VMEM((4, J, w), F32),
        pltpu.VMEM((4, J, w), F32),
        pltpu.VMEM((4, J, w), F32),
        pltpu.VMEM((4, J, w), F32),
        pltpu.VMEM((4, J, w), F32),
        pltpu.VMEM((4, 8, users), F32),
        pltpu.VMEM((users, emb), F32),
        pltpu.VMEM((4, emb, users), BF16),
        pltpu.VMEM((8, 128), F32),
        pltpu.VMEM((users, emb), F32),
        dma((NSLOT,)), dma,
        dma((3, J)), dma((3, J)),
        dma((3, J)), dma((3, J)),
        dma((3, J)), dma((3, J)),
        dma((3, J)), dma((3, J)),
        dma((3, J)), dma((3, J)),
        dma((5, 3)), dma((5, 3)),
        dma((4,)), dma((4,)), dma((4,)), dma((4,)),
        dma((3,)), dma((3,)),
    ]
    vm, hbm = pl.BlockSpec(memory_space=pltpu.VMEM), pl.BlockSpec(memory_space=pl.ANY)
    return pl.pallas_call(
        kern,
        out_shape=(jax.ShapeDtypeStruct((shard_users, emb), BF16),
                   jax.ShapeDtypeStruct((J, emb, w), BF16),
                   jax.ShapeDtypeStruct((emb, n_query), BF16)),
        in_specs=[hbm, hbm, vm, vm],
        out_specs=(vm, vm, vm),
        scratch_shapes=scratch,
        name='propagate',
        compiler_params=pltpu.CompilerParams(
            collective_id=0, has_side_effects=True, vmem_limit_bytes=60 * 2 ** 20))


def score_kernel(qt, fit, scores, final_item):
    f = fit[0]
    scores[...] = lax.dot_general(qt[...], f, (((0,), (0,)), ((), ())), preferred_element_type=F32)
    final_item[...] = jnp.transpose(f.astype(F32)).astype(BF16)


def score(qt, fit):
    emb, n_query = qt.shape
    n, _, w = fit.shape
    return pl.pallas_call(
        score_kernel,
        grid=(n,),
        out_shape=(jax.ShapeDtypeStruct((n_query, n * w), F32), jax.ShapeDtypeStruct((n * w, emb), BF16)),
        in_specs=[pl.BlockSpec((emb, n_query), lambda j: (0, 0)), pl.BlockSpec((1, emb, w), lambda j: (j, 0, 0))],
        out_specs=(pl.BlockSpec((n_query, w), lambda j: (0, j)), pl.BlockSpec((w, emb), lambda j: (j, 0))),
        name='score',
    )(qt, fit)


def solution(mesh):
    def device_step(mask_blk, user_shard, item_shard, queries):
        users, width = mask_blk.shape
        quarter, emb = item_shard.shape
        n_query = queries.shape[0]
        call = make_kernel(users, width, quarter, emb, user_shard.shape[0], n_query)
        final_user, fit, qt = call(mask_blk, item_shard, user_shard, queries.reshape(1, n_query))
        scores, final_item = score(qt, fit)
        return final_user, final_item, scores

    return jax.shard_map(device_step, mesh=mesh, in_specs=(P('row', 'col'), P(('row', 'col'), None), P(('col', 'row'), None), P()), out_specs=(P(('row', 'col'), None), P(('col', 'row'), None), P(None, ('col', 'row'))), check_vma=False)
```

```python
import jax
import jax.numpy as jnp
from jax import lax
from jax.experimental import pallas as pl
from jax.experimental.pallas import tpu as pltpu
from jax.sharding import PartitionSpec as P

LAYERS = 3
J = 8
NSLOT = 8
HEAD = 5
EARLY = 5
FIRST = 5
VMEM_MIB = 52
HALF = 2
F32, BF16 = jnp.float32, jnp.bfloat16


def nt(a, b):
    return lax.dot_general(a, b, (((1,), (1,)), ((), ())), preferred_element_type=F32)


def nn(a, b):
    return lax.dot_general(a, b, (((1,), (0,)), ((), ())), preferred_element_type=F32)


def remote(src, dst, send, recv, **where):
    return pltpu.make_async_remote_copy(
        src_ref=src, dst_ref=dst, send_sem=send, recv_sem=recv,
        device_id=where, device_id_type=pl.DeviceIdType.MESH)


def make_kernel(users, width, quarter, emb, shard_users, n_query):
    w = quarter // J
    piece = quarter // HALF
    rows_blk = 64
    n_rb = users // rows_blk
    lanes = w // 128

    def kern(mask, item, user, queries, fu_out, fit, q_out,
             adj, stage, panel, ps, pk, rs, rx, isum, ut, u0t, usend, urecv, usum,
             rowacc, invu, di, di_sib, di_chip, di_x, di_dg, invi, du, acc, fut, qrow,
             m_sem, i_sem, in_sem, ps_s, ps_r0, ps_r1, tx_s, tx_r, as_s, as_r, ax_s, ax_r, af_s, af_r,
             u_s, u_r, d_s, d_r, dx_s, dx_r, l_s, l_r, f_s, f_r):
        r = lax.axis_index('row')
        c = lax.axis_index('col')
        sib = r + 1 - 2 * (r % 2)
        xp = (r + 2) % 4
        dg = (sib + 2) % 4
        cols = [(c + k) % 4 for k in (1, 2, 3)]

        def over(n, body, start=0):
            def step(j, carry):
                body(j)
                return carry
            lax.fori_loop(start, n, step, 0)

        def part_of(j):
            return pl.ds(pl.multiple_of(j * w, w), w)

        def piece_of(h):
            return pl.ds(pl.multiple_of(h * piece, piece), piece)

        def mask_copy(b):
            return pltpu.make_async_copy(
                mask.at[:, pl.ds(pl.multiple_of(b * w, w), w)], stage.at[b % NSLOT], m_sem.at[b % NSLOT])

        item_copy = pltpu.make_async_copy(item, panel.at[0, r], i_sem)
        item_copy.start()
        user_copy = pltpu.make_async_copy(user, u0t.at[c], in_sem.at[0])
        user_copy.start()
        query_copy = pltpu.make_async_copy(queries, qrow, in_sem.at[1])
        query_copy.start()
        for b in range(NSLOT):
            mask_copy(b).start()

        bar = pltpu.get_barrier_semaphore()
        for q in (sib, xp, dg):
            pl.semaphore_signal(bar, inc=1, device_id={'row': q}, device_id_type=pl.DeviceIdType.MESH)
        for q in cols:
            pl.semaphore_signal(bar, inc=1, device_id={'col': q}, device_id_type=pl.DeviceIdType.MESH)

        def to_sib(src, dst, send, recv):
            return remote(src, dst, send, recv, row=sib)

        def to_xp(src, dst, send, recv):
            return remote(src, dst, send, recv, row=xp)

        def ps_near(s, j):
            return to_sib(ps.at[0, j], rs.at[s, 0, j], ps_s, ps_r0.at[s % 2])

        def ps_far(s, j):
            return to_sib(ps.at[1, j], rs.at[s, 1, j], ps_s, ps_r1.at[s % 2, j])

        def ps_near_all(s):
            return to_sib(ps.at[0], rs.at[s, 0], ps_s, ps_r0.at[s % 2])

        def ps_all(s):
            return to_sib(ps, rs.at[s], ps_s, ps_r0.at[s % 2])

        def tx_copy(s, j):
            return to_xp(pk.at[1, j], rx.at[s, j], tx_s, tx_r.at[s % 2, j])

        def tx_all(s):
            return to_xp(pk.at[1], rx.at[s], tx_s, tx_r.at[s % 2, 0])

        def as_copy(s, sl, q):
            ref = panel.at[s, q, :, sl]
            return to_sib(ref, ref, as_s.at[s % 2], as_r.at[s % 2])

        def ax_copy(s, sl, q, h):
            ref = panel.at[s, q, :, sl]
            return to_xp(ref, ref, ax_s.at[s % 2], ax_r.at[s % 2, h])

        def af_copy(s, sl, q, h):
            ref = panel.at[s, q, :, sl]
            return to_sib(ref, ref, af_s.at[s % 2], af_r.at[s % 2, h])

        whole = pl.ds(0, quarter)

        def share_far(s, j):
            ax_copy(s, part_of(j), r, j // (J // HALF)).start()

        def share_item(s, j):
            as_copy(s, part_of(j), r).start()
            share_far(s, j)

        def user_copies(kind, src, dst, slot):
            return [remote(src, dst.at[slot], u_s.at[kind], u_r.at[kind], col=q) for q in cols]

        def user_all(kind, buf):
            three = buf.at[pl.ds(0, 3)]
            return remote(three, three, u_s.at[kind], u_r.at[kind], col=cols[0])

        def dis_copy(q):
            return to_sib(di.at[q], di_sib.at[q], d_s, d_r.at[q])

        def dix_copy(q):
            return to_xp(di_chip.at[q], di_x.at[q], dx_s, dx_r.at[q])

        def chip_degree(q):
            dis_copy(q).wait_recv()
            di_chip[q] = di[q] + di_sib[q]
            dix_copy(q).start()

        rowacc[...] = jnp.zeros_like(rowacc)

        def mask_pass(q, first=0, last=J):
            def mask_step(j):
                b = q * J + j
                mask_copy(b).wait()
                slot = b % NSLOT

                def rows_step(rb, csum):
                    rows = pl.ds(pl.multiple_of(rb * rows_blk, rows_blk), rows_blk)
                    m = stage[slot, rows, :].astype(F32)
                    adj[q, rows, part_of(j)] = m.astype(BF16)
                    part = m[:, :128]
                    for t in range(1, lanes):
                        part = part + m[:, t * 128:(t + 1) * 128]
                    rowacc[rows, :] = rowacc[rows, :] + part
                    for t in range(0, rows_blk, 8):
                        csum = csum + m[t:t + 8, :]
                    return csum

                csum = lax.fori_loop(0, n_rb, rows_step, jnp.zeros((8, w), F32), unroll=2)
                di[q, pl.ds(j, 1), :] = jnp.sum(csum, axis=0, keepdims=True)

                @pl.when(b + NSLOT < 4 * J)
                def _():
                    mask_copy(b + NSLOT).start()

            over(last, mask_step, first)

        with jax.named_scope('mask_0'):
            mask_pass(0, 0, HEAD)
        with jax.named_scope('first_item'):
            item_copy.wait()
            pl.semaphore_wait(bar, 6)
            user_copy.wait()
            query_copy.wait()
            for cp in user_copies(0, u0t.at[c], u0t, c):
                cp.start()
            as_copy(0, whole, r).start()
            over(EARLY, lambda j: share_far(0, j))
        with jax.named_scope('mask_0b'):
            mask_pass(0, HEAD)
        dis_copy(0).start()
        for q in range(1, 4):
            with jax.named_scope(f'mask_{q}'):
                mask_pass(q)
            if q < 3:
                dis_copy(q).start()
            chip_degree(q - 1)

        with jax.named_scope('degrees'):
            last_di = [to_sib(di.at[3], di_sib.at[3], l_s, d_r.at[3]), to_xp(di.at[3], di_x.at[3], l_s, dx_r.at[3]),
                       remote(di.at[3], di_dg, l_s, l_r, row=dg)]
            for cp in last_di:
                cp.start()
            over(J, lambda j: share_far(0, j), EARLY)
            du[c] = nt(jnp.ones((8, 128), BF16), rowacc[...].astype(BF16))
            for cp in user_copies(4, du.at[c], du, c):
                cp.start()
            user_all(0, u0t).wait_recv()
            u0 = jnp.concatenate([u0t[k] for k in range(4)], axis=1)
            ut[...] = u0
            usum[...] = u0.astype(F32)
            with jax.named_scope('wait_di'):
                for q in range(3):
                    dix_copy(q).wait_recv()
                    invi[q] = lax.rsqrt(jnp.maximum(di_chip[q] + di_x[q], 1.0))
                for cp in last_di:
                    cp.wait_recv()
                invi[3] = lax.rsqrt(jnp.maximum((di[3] + di_sib[3]) + (di_x[3] + di_dg[...]), 1.0))
            with jax.named_scope('wait_du'):
                user_all(4, du).wait_recv()
            deg = ((du[0] + du[1]) + du[2]) + du[3]
            inv_row = lax.rsqrt(jnp.maximum(deg, 1.0))
            invu[...] = jnp.transpose(jnp.broadcast_to(inv_row[0:1, :], (128, users)))

        def form(q, j):
            def rows_step(rb, carry):
                rows = pl.ds(pl.multiple_of(rb * rows_blk, rows_blk), rows_blk)
                m = adj[q, rows, part_of(j)].astype(F32)
                iu = jnp.concatenate([invu[rows, :]] * lanes, axis=1)
                adj[q, rows, part_of(j)] = ((iu * m) * invi[q, pl.ds(j, 1), :]).astype(BF16)
                return carry

            lax.fori_loop(0, n_rb, rows_step, 0, unroll=2)

        def sum_far(s, j):
            ps_far(s, j).wait_recv()
            pk[1, j] = pk[1, j] + rs[s, 1, j]

        def item_part(s):
            def term(q, j):
                if s == 0:
                    form(q, j)
                return nn(ut[...], adj[q, :, part_of(j)])

            def step(j):
                ps[1, j] = term(dg, j)
                ps_far(s, j).start()
                pk[1, j] = term(xp, j)
                ps[0, j] = term(sib, j)
                ps_near(s, j).start()
                pk[0, j] = term(r, j)
                if s == 0:
                    sum_far(s, j)
                    tx_copy(s, j).start()
                elif s == 1:
                    @pl.when(j > 0)
                    def _():
                        sum_far(s, j - 1)
                        tx_copy(s, j - 1).start()
                else:
                    @pl.when(j > 0)
                    def _():
                        sum_far(s, j - 1)

                    @pl.when((j > 0) & (j <= FIRST))
                    def _():
                        tx_copy(s, j - 1).start()

            over(J, step)
            if s:
                sum_far(s, J - 1)
            if s == 1:
                tx_copy(s, J - 1).start()

        def item_finish(s):
            ps_near_all(s).wait_recv()

            def step(j):
                tx_copy(s, j).wait_recv()
                v = ((pk[0, j] + rs[s, 0, j]) + rx[s, j]).astype(BF16)
                before = panel[0, r, :, part_of(j)].astype(F32) if s == 0 else isum[j]
                total = before + v.astype(F32)
                if s < LAYERS - 1:
                    panel[s + 1, r, :, part_of(j)] = v
                    share_item(s + 1, j)
                    isum[j] = total
                else:
                    fit[j] = (total / (LAYERS + 1)).astype(BF16)

            over(J, step)

        def drain(s):
            ps_all(s).wait_send()
            as_copy(s, whole, r).wait_send()
            ax_copy(s, whole, r, 0).wait_send()
            af_copy(s, whole, xp, 0).wait_send()

        def user_part(s):
            def add(q, h):
                acc[...] = acc[...] + nt(adj[q, :, piece_of(h)], panel[s, q, :, piece_of(h)])

            acc[...] = jnp.zeros_like(acc)
            over(HALF, lambda h: add(r, h))
            as_copy(s, whole, sib).wait_recv()
            over(HALF, lambda h: add(sib, h))

            def far(h):
                ax_copy(s, piece_of(h), xp, h).wait_recv()
                af_copy(s, piece_of(h), xp, h).start()
                add(xp, h)
                af_copy(s, piece_of(h), dg, h).wait_recv()
                add(dg, h)

            over(HALF, far)
            t = jnp.transpose(acc[...])
            usend[s] = t
            urecv[s, c] = t
            for cp in user_copies(s + 1, usend.at[s], urecv.at[s], c):
                cp.start()

        def user_finish(s):
            user_all(s + 1, urecv.at[s]).wait_recv()
            v = (((urecv[s, 0] + urecv[s, 1]) + urecv[s, 2]) + urecv[s, 3]).astype(BF16)
            ut[...] = v
            usum[...] = usum[...] + v.astype(F32)

        for s in range(LAYERS):
            with jax.named_scope(f'item_part_{s}'):
                item_part(s)
            with jax.named_scope(f'user_part_{s}'):
                user_part(s)
            if s < LAYERS - 1:
                with jax.named_scope(f'item_finish_{s}'):
                    item_finish(s)
                    tx_all(s).wait_send()
            with jax.named_scope(f'user_finish_{s}'):
                drain(s)
                user_finish(s)

        with jax.named_scope('final_users'):
            fu = (usum[...] / (LAYERS + 1)).astype(BF16)
            for k in range(4):
                fut[r, k] = fu[:, k * shard_users:(k + 1) * shard_users]
            fu_out[...] = fut[r, c]
            cross = to_xp(fut.at[r, c], fut.at[r, c], f_s.at[0], f_r.at[0])
            cross.start()
            over(J, lambda j: tx_copy(2, j).start(), FIRST)
            own = to_sib(fut.at[r], fut.at[r], f_s.at[1], f_r.at[1])
            own.start()
            cross.wait_recv()
            spread = [remote(fut.at[xp, c], fut.at[xp, c], f_s.at[2], f_r.at[2], col=q) for q in cols]
            for cp in spread:
                cp.start()
            three = fut.at[xp, pl.ds(0, 3)]
            spread_all = remote(three, three, f_s.at[2], f_r.at[2], col=cols[0])
            spread_all.wait_recv()
            other = to_sib(fut.at[xp], fut.at[xp], f_s.at[3], f_r.at[3])
            other.start()
            own.wait_recv()
            other.wait_recv()
            qt = jnp.zeros((emb, n_query), F32)
            for q in range(4):
                ids = lax.broadcasted_iota(jnp.int32, (users, n_query), 0) + q * users
                onehot = jnp.where(ids == qrow[...], 1.0, 0.0).astype(BF16)
                qt = qt + nn(jnp.concatenate([fut[q, k] for k in range(4)], axis=1), onehot)
            q_out[...] = jnp.transpose(qt).astype(BF16)

            user_all(0, u0t).wait_send()
            user_all(4, du).wait_send()
            for s in range(3):
                user_all(s + 1, urecv.at[s]).wait_send()
            three = pl.ds(0, 3)
            to_sib(di.at[three], di_sib.at[three], d_s, d_r.at[0]).wait_send()
            to_xp(di_chip.at[three], di_x.at[three], dx_s, dx_r.at[0]).wait_send()
            to_sib(di.at[three], di_sib.at[three], l_s, d_r.at[0]).wait_send()
            cross.wait_send()
            own.wait_send()
            spread_all.wait_send()
            other.wait_send()
        with jax.named_scope('item_finish_2'):
            item_finish(2)
        with jax.named_scope('end'):
            tx_all(2).wait_send()

    dma = pltpu.SemaphoreType.DMA
    scratch = [
        pltpu.VMEM((4, users, quarter), BF16),
        pltpu.VMEM((NSLOT, users, w), jnp.int32),
        pltpu.VMEM((3, 4, emb, quarter), BF16),
        pltpu.VMEM((2, J, emb, w), F32),
        pltpu.VMEM((2, J, emb, w), F32),
        pltpu.VMEM((3, 2, J, emb, w), F32),
        pltpu.VMEM((3, J, emb, w), F32),
        pltpu.VMEM((J, emb, w), F32),
        pltpu.VMEM((emb, users), BF16),
        pltpu.VMEM((4, emb, shard_users), BF16),
        pltpu.VMEM((3, emb, users), F32),
        pltpu.VMEM((3, 4, emb, users), F32),
        pltpu.VMEM((emb, users), F32),
        pltpu.VMEM((users, 128), F32),
        pltpu.VMEM((users, 128), F32),
        pltpu.VMEM((4, J, w), F32),
        pltpu.VMEM((4, J, w), F32),
        pltpu.VMEM((4, J, w), F32),
        pltpu.VMEM((4, J, w), F32),
        pltpu.VMEM((J, w), F32),
        pltpu.VMEM((4, J, w), F32),
        pltpu.VMEM((4, 8, users), F32),
        pltpu.VMEM((users, emb), F32),
        pltpu.VMEM((4, 4, emb, shard_users), BF16),
        pltpu.VMEM((1, n_query), jnp.int32),
        dma((NSLOT,)), dma, dma((2,)),
        dma, dma((2,)), dma((2, J)),
        dma, dma((2, J)),
        dma((2,)), dma((2,)),
        dma((2,)), dma((2, HALF)),
        dma((2,)), dma((2, HALF)),
        dma((5,)), dma((5,)),
        dma, dma((4,)), dma, dma((4,)), dma, dma,
        dma((4,)), dma((4,)),
    ]
    vm, hbm = pl.BlockSpec(memory_space=pltpu.VMEM), pl.BlockSpec(memory_space=pltpu.HBM)
    return pl.pallas_call(
        kern,
        out_shape=(jax.ShapeDtypeStruct((emb, shard_users), BF16),
                   jax.ShapeDtypeStruct((J, emb, w), BF16),
                   jax.ShapeDtypeStruct((n_query, emb), BF16)),
        in_specs=[hbm, hbm, hbm, hbm],
        out_specs=(vm, vm, vm),
        scratch_shapes=scratch,
        name='propagate',
        compiler_params=pltpu.CompilerParams(
            collective_id=0, has_side_effects=True, vmem_limit_bytes=VMEM_MIB * 2 ** 20))


def score_kernel(query, fit, fu, scores, item_out, user_out, buf, s_sem, i_sem, u_sem):
    n, _, w = fit.shape
    pltpu.make_async_copy(fu, user_out, u_sem).start()

    def cols(j):
        return pl.ds(pl.multiple_of(j * w, w), w)

    def score_copy(j):
        return pltpu.make_async_copy(buf.at[j], scores.at[:, cols(j)], s_sem.at[j])

    def item_copy(j):
        return pltpu.make_async_copy(fit.at[j], item_out.at[:, cols(j)], i_sem.at[j])

    def step(j, carry):
        buf[j] = nn(query[...], fit[j])
        score_copy(j).start()
        item_copy(j).start()
        return carry

    def finish(j, carry):
        score_copy(j).wait()
        item_copy(j).wait()
        return carry

    lax.fori_loop(0, n, step, 0)
    lax.fori_loop(0, n, finish, 0)
    pltpu.make_async_copy(fu, user_out, u_sem).wait()


def score(query, fit, fu):
    n_query, emb = query.shape
    n, _, w = fit.shape
    vm, hbm = pl.BlockSpec(memory_space=pltpu.VMEM), pl.BlockSpec(memory_space=pl.ANY)
    return pl.pallas_call(
        score_kernel,
        out_shape=(jax.ShapeDtypeStruct((n_query, n * w), F32), jax.ShapeDtypeStruct((emb, n * w), BF16),
                   jax.ShapeDtypeStruct(fu.shape, BF16)),
        in_specs=[vm, vm, vm],
        out_specs=(hbm, hbm, hbm),
        scratch_shapes=[pltpu.VMEM((n, n_query, w), F32), pltpu.SemaphoreType.DMA((n,)),
                        pltpu.SemaphoreType.DMA((n,)), pltpu.SemaphoreType.DMA],
        name='score',
        compiler_params=pltpu.CompilerParams(vmem_limit_bytes=12 * 2 ** 20),
    )(query, fit, fu)


def solution(mesh):
    def device_step(mask_blk, user_shard, item_shard, queries):
        users, width = mask_blk.shape
        quarter, emb = item_shard.shape
        n_query = queries.shape[0]
        call = make_kernel(users, width, quarter, emb, user_shard.shape[0], n_query)
        fu, fit, query = call(*[pltpu.with_memory_space_constraint(a, pltpu.HBM) for a in (
            mask_blk, item_shard.T, user_shard.T, queries.reshape(1, n_query))])
        scores, final_item, final_user = score(query, fit, fu)
        return final_user.T, final_item.T, scores

    return jax.shard_map(device_step, mesh=mesh, in_specs=(P('row', 'col'), P(('row', 'col'), None), P(('col', 'row'), None), P()), out_specs=(P(('row', 'col'), None), P(('col', 'row'), None), P(None, ('col', 'row'))), check_vma=False)
```

```python
import jax
import jax.numpy as jnp
from jax import lax
from jax.experimental import pallas as pl
from jax.experimental.pallas import tpu as pltpu
from jax.sharding import PartitionSpec as P

LAYERS = 3
J = 8
NSLOT = 8
HEAD = 2
NEXT = 5
LEAD = 2
EARLY = 5
FIRST = 5
VMEM_MIB = 52
HALF = 2
F32, BF16 = jnp.float32, jnp.bfloat16


def nt(a, b):
    return lax.dot_general(a, b, (((1,), (1,)), ((), ())), preferred_element_type=F32)


def nn(a, b):
    return lax.dot_general(a, b, (((1,), (0,)), ((), ())), preferred_element_type=F32)


def remote(src, dst, send, recv, **where):
    return pltpu.make_async_remote_copy(
        src_ref=src, dst_ref=dst, send_sem=send, recv_sem=recv,
        device_id=where, device_id_type=pl.DeviceIdType.MESH)


def make_kernel(users, width, quarter, emb, shard_users, n_query):
    w = quarter // J
    piece = quarter // HALF
    rows_blk = 64
    n_rb = users // rows_blk
    lanes = w // 128

    def kern(mask, item, user, queries, fu_out, fit, q_out,
             adj, stage, panel, ps, pk, rs, rx, isum, ut, u0t, usend, urecv, usum,
             rowacc, invu, di, di_sib, di_chip, di_x, di_dg, invi, du, acc, fut, qrow,
             m_sem, i_sem, in_sem, ps_s, ps_r0, ps_r1, ps_rh, tx_s, tx_r, as_s, as_r, ax_s, ax_r, af_s, af_r,
             u_s, u_r, d_s, d_r, dx_s, dx_r, l_s, l_r, f_s, f_r):
        r = lax.axis_index('row')
        c = lax.axis_index('col')
        sib = r + 1 - 2 * (r % 2)
        xp = (r + 2) % 4
        dg = (sib + 2) % 4
        cols = [(c + k) % 4 for k in (1, 2, 3)]

        def over(n, body, start=0):
            def step(j, carry):
                body(j)
                return carry
            lax.fori_loop(start, n, step, 0)

        def part_of(j):
            return pl.ds(pl.multiple_of(j * w, w), w)

        def piece_of(h):
            return pl.ds(pl.multiple_of(h * piece, piece), piece)

        def mask_copy(b):
            return pltpu.make_async_copy(
                mask.at[:, pl.ds(pl.multiple_of(b * w, w), w)], stage.at[b % NSLOT], m_sem.at[b % NSLOT])

        lead = LEAD * w

        def item_copy(k):
            sl = (pl.ds(0, lead), pl.ds(lead, quarter - lead))[k]
            return pltpu.make_async_copy(item.at[:, sl], panel.at[0, r, :, sl], i_sem.at[k])

        for k in range(2):
            item_copy(k).start()
        user_copy = pltpu.make_async_copy(user, u0t.at[c], in_sem.at[0])
        user_copy.start()
        query_copy = pltpu.make_async_copy(queries, qrow, in_sem.at[1])
        query_copy.start()
        for b in range(NSLOT):
            mask_copy(b).start()

        bar = pltpu.get_barrier_semaphore()
        for q in (sib, xp, dg):
            pl.semaphore_signal(bar, inc=1, device_id={'row': q}, device_id_type=pl.DeviceIdType.MESH)
        for q in cols:
            pl.semaphore_signal(bar, inc=1, device_id={'col': q}, device_id_type=pl.DeviceIdType.MESH)

        def to_sib(src, dst, send, recv):
            return remote(src, dst, send, recv, row=sib)

        def to_xp(src, dst, send, recv):
            return remote(src, dst, send, recv, row=xp)

        def ps_near(s, j):
            return to_sib(ps.at[0, j], rs.at[s, 0, j], ps_s, ps_r0.at[s % 2])

        def ps_far(s, j):
            return to_sib(ps.at[1, j], rs.at[s, 1, j], ps_s, ps_r1.at[j])

        def ps_near_all(s):
            return to_sib(ps.at[0], rs.at[s, 0], ps_s, ps_r0.at[s % 2])

        def ps_all(s):
            return to_sib(ps, rs.at[s], ps_s, ps_r0.at[s % 2])

        def tx_copy(s, j):
            return to_xp(pk.at[1, j], rx.at[s, j], tx_s, tx_r.at[s % 2, j // 2])

        def tx_pair(s, i):
            two = pl.ds(2 * i, 2)
            return to_xp(pk.at[1, two], rx.at[s, two], tx_s, tx_r.at[s % 2, i])

        def tx_all(s):
            return to_xp(pk.at[1], rx.at[s], tx_s, tx_r.at[s % 2, 0])

        def as_copy(s, sl, q):
            ref = panel.at[s, q, :, sl]
            return to_sib(ref, ref, as_s, as_r)

        def ax_copy(s, sl, q, h):
            ref = panel.at[s, q, :, sl]
            return to_xp(ref, ref, ax_s, ax_r.at[s % 2, h])

        def af_copy(s, sl, q, h):
            ref = panel.at[s, q, :, sl]
            return to_sib(ref, ref, af_s, af_r.at[h])

        whole = pl.ds(0, quarter)

        def share_far(s, j):
            ax_copy(s, part_of(j), r, j // (J // HALF)).start()

        def share_item(s, j):
            as_copy(s, part_of(j), r).start()
            share_far(s, j)

        def user_copies(kind, src, dst, slot):
            return [remote(src, dst.at[slot], u_s, u_r.at[kind], col=q) for q in cols]

        def user_all(kind, buf):
            three = buf.at[pl.ds(0, 3)]
            return remote(three, three, u_s, u_r.at[kind], col=cols[0])

        def dis_copy(q):
            return to_sib(di.at[q], di_sib.at[q], d_s, d_r.at[q])

        def dix_copy(q):
            return to_xp(di_chip.at[q], di_x.at[q], dx_s, dx_r.at[q])

        def chip_degree(q):
            dis_copy(q).wait_recv()
            di_chip[q] = di[q] + di_sib[q]
            dix_copy(q).start()

        rowacc[...] = jnp.zeros_like(rowacc)

        def mask_pass(q, first=0, last=J):
            def mask_step(j):
                b = q * J + j
                mask_copy(b).wait()
                slot = b % NSLOT

                def rows_step(rb, csum):
                    rows = pl.ds(pl.multiple_of(rb * rows_blk, rows_blk), rows_blk)
                    m = stage[slot, rows, :].astype(F32)
                    adj[q, rows, part_of(j)] = m.astype(BF16)
                    part = m[:, :128]
                    for t in range(1, lanes):
                        part = part + m[:, t * 128:(t + 1) * 128]
                    rowacc[rows, :] = rowacc[rows, :] + part
                    for t in range(0, rows_blk, 8):
                        csum = csum + m[t:t + 8, :]
                    return csum

                csum = lax.fori_loop(0, n_rb, rows_step, jnp.zeros((8, w), F32), unroll=2)
                di[q, pl.ds(j, 1), :] = jnp.sum(csum, axis=0, keepdims=True)

                @pl.when(b + NSLOT < 4 * J)
                def _():
                    mask_copy(b + NSLOT).start()

            over(last, mask_step, first)

        with jax.named_scope('mask_0'):
            mask_pass(0, 0, HEAD)
        with jax.named_scope('first_item'):
            item_copy(0).wait()
            pl.semaphore_wait(bar, 6)
            over(LEAD, lambda j: share_far(0, j))
        with jax.named_scope('mask_0b'):
            mask_pass(0, HEAD, NEXT)
            item_copy(1).wait()
            over(EARLY, lambda j: share_far(0, j), LEAD)
            as_copy(0, whole, r).start()
            user_copy.wait()
            query_copy.wait()
            for cp in user_copies(0, u0t.at[c], u0t, c):
                cp.start()
            mask_pass(0, NEXT)
        dis_copy(0).start()
        for q in range(1, 4):
            with jax.named_scope(f'mask_{q}'):
                mask_pass(q)
            if q < 3:
                dis_copy(q).start()
            chip_degree(q - 1)

        with jax.named_scope('degrees'):
            last_di = [to_sib(di.at[3], di_sib.at[3], l_s, d_r.at[3]), to_xp(di.at[3], di_x.at[3], l_s, dx_r.at[3]),
                       remote(di.at[3], di_dg, l_s, l_r, row=dg)]
            for cp in last_di:
                cp.start()
            over(J, lambda j: share_far(0, j), EARLY)
            user_all(0, u0t).wait_send()
            du[c] = nt(jnp.ones((8, 128), BF16), rowacc[...].astype(BF16))
            for cp in user_copies(4, du.at[c], du, c):
                cp.start()
            user_all(0, u0t).wait_recv()
            u0 = jnp.concatenate([u0t[k] for k in range(4)], axis=1)
            ut[...] = u0
            usum[...] = u0.astype(F32)
            with jax.named_scope('wait_di'):
                for q in range(3):
                    dix_copy(q).wait_recv()
                    invi[q] = lax.rsqrt(jnp.maximum(di_chip[q] + di_x[q], 1.0))
                for cp in last_di:
                    cp.wait_recv()
                invi[3] = lax.rsqrt(jnp.maximum((di[3] + di_sib[3]) + (di_x[3] + di_dg[...]), 1.0))
            with jax.named_scope('wait_du'):
                user_all(4, du).wait_recv()
            deg = ((du[0] + du[1]) + du[2]) + du[3]
            inv_row = lax.rsqrt(jnp.maximum(deg, 1.0))
            invu[...] = jnp.transpose(jnp.broadcast_to(inv_row[0:1, :], (128, users)))

        def form(q, j, off=0, n=w):
            def rows_step(rb, carry):
                rows = pl.ds(pl.multiple_of(rb * rows_blk, rows_blk), rows_blk)
                at = pl.ds(pl.multiple_of(j * w + off, n), n)
                m = adj[q, rows, at].astype(F32)
                iu = jnp.concatenate([invu[rows, :]] * (n // 128), axis=1)
                adj[q, rows, at] = ((iu * m) * invi[q, pl.ds(j, 1), off:off + n]).astype(BF16)
                return carry

            lax.fori_loop(0, n_rb, rows_step, 0, unroll=2)

        def sum_far(s, j):
            ps_far(s, j).wait_recv()
            pk[1, j] = pk[1, j] + rs[s, 1, j]

        def first_part():
            half = w // 2
            sls = [slice(h * half, (h + 1) * half) for h in range(2)]
            ends = [ps_rh, ps_r1.at[0]]

            def half_copy(h):
                return to_sib(ps.at[1, 0, :, sls[h]], rs.at[0, 1, 0, :, sls[h]], ps_s, ends[h])

            for h in range(2):
                form(dg, 0, h * half, half)
                ps[1, 0, :, sls[h]] = nn(ut[...], adj[dg, :, sls[h]])
                half_copy(h).start()
            form(xp, 0)
            pk[1, 0] = nn(ut[...], adj[xp, :, part_of(0)])
            form(sib, 0)
            ps[0, 0] = nn(ut[...], adj[sib, :, part_of(0)])
            ps_near(0, 0).start()
            for h in range(2):
                half_copy(h).wait_recv()
                pk[1, 0, :, sls[h]] = pk[1, 0, :, sls[h]] + rs[0, 1, 0, :, sls[h]]
                to_xp(pk.at[1, 0, :, sls[h]], rx.at[0, 0, :, sls[h]], tx_s, tx_r.at[0, 0]).start()
            form(r, 0)
            pk[0, 0] = nn(ut[...], adj[r, :, part_of(0)])

        def item_part(s):
            def term(q, j):
                if s == 0:
                    form(q, j)
                return nn(ut[...], adj[q, :, part_of(j)])

            def step(j):
                ps[1, j] = term(dg, j)
                ps_far(s, j).start()
                pk[1, j] = term(xp, j)
                ps[0, j] = term(sib, j)
                ps_near(s, j).start()
                pk[0, j] = term(r, j)
                if s == 0:
                    sum_far(s, j)
                    tx_copy(s, j).start()
                elif s == 1:
                    @pl.when(j > 0)
                    def _():
                        sum_far(s, j - 1)
                        tx_copy(s, j - 1).start()
                else:
                    @pl.when(j > 0)
                    def _():
                        sum_far(s, j - 1)

                    @pl.when((j > 0) & (j <= FIRST))
                    def _():
                        tx_copy(s, j - 1).start()

            if s == 0:
                first_part()
            over(J, step, 0 if s else 1)
            if s:
                sum_far(s, J - 1)
            if s == 1:
                tx_copy(s, J - 1).start()

        def item_finish(s):
            ps_near_all(s).wait_recv()

            def finish(j):
                v = ((pk[0, j] + rs[s, 0, j]) + rx[s, j]).astype(BF16)
                before = panel[0, r, :, part_of(j)].astype(F32) if s == 0 else isum[j]
                total = before + v.astype(F32)
                if s < LAYERS - 1:
                    panel[s + 1, r, :, part_of(j)] = v
                    share_item(s + 1, j)
                    isum[j] = total
                else:
                    fit[j] = (total / (LAYERS + 1)).astype(BF16)

            def step(i):
                tx_pair(s, i).wait_recv()
                finish(2 * i)
                finish(2 * i + 1)

            over(J // 2, step)

        def drain(s):
            as_copy(s, whole, r).wait_send()
            ax_copy(s, whole, r, 0).wait_send()

        def user_part(s):
            def add(q, h):
                acc[...] = acc[...] + nt(adj[q, :, piece_of(h)], panel[s, q, :, piece_of(h)])

            acc[...] = jnp.zeros_like(acc)
            over(HALF, lambda h: add(r, h))
            as_copy(s, whole, sib).wait_recv()
            over(HALF, lambda h: add(sib, h))

            def far(h):
                ax_copy(s, piece_of(h), xp, h).wait_recv()
                af_copy(s, piece_of(h), xp, h).start()
                add(xp, h)
                af_copy(s, piece_of(h), dg, h).wait_recv()
                add(dg, h)

            over(HALF, far)
            if s == 0:
                user_all(4, du).wait_send()
            t = jnp.transpose(acc[...])
            usend[s] = t
            urecv[s, c] = t
            for cp in user_copies(s + 1, usend.at[s], urecv.at[s], c):
                cp.start()

        def user_finish(s):
            user_all(s + 1, urecv.at[s]).wait_recv()
            user_all(s + 1, urecv.at[s]).wait_send()
            v = (((urecv[s, 0] + urecv[s, 1]) + urecv[s, 2]) + urecv[s, 3]).astype(BF16)
            ut[...] = v
            usum[...] = usum[...] + v.astype(F32)

        for s in range(LAYERS):
            with jax.named_scope(f'item_part_{s}'):
                item_part(s)
            with jax.named_scope(f'user_part_{s}'):
                user_part(s)
                drain(s)
            if s < LAYERS - 1:
                with jax.named_scope(f'item_finish_{s}'):
                    item_finish(s)
                    tx_all(s).wait_send()
            with jax.named_scope(f'user_finish_{s}'):
                ps_all(s).wait_send()
                af_copy(s, whole, xp, 0).wait_send()
                user_finish(s)

        with jax.named_scope('final_users'):
            fu = (usum[...] / (LAYERS + 1)).astype(BF16)
            for k in range(4):
                fut[r, k] = fu[:, k * shard_users:(k + 1) * shard_users]
            fu_out[...] = fut[r, c]
            cross = to_xp(fut.at[r, c], fut.at[r, c], f_s, f_r.at[0])
            cross.start()
            over(J - 1, lambda j: tx_copy(2, j).start(), FIRST)

            @pl.when(r % 2 == 0)
            def _():
                tx_copy(2, J - 1).start()
            own = to_sib(fut.at[r], fut.at[r], f_s, f_r.at[1])
            own.start()
            cross.wait_recv()
            spread = [remote(fut.at[xp, c], fut.at[xp, c], f_s, f_r.at[2], col=q) for q in cols]
            for cp in spread:
                cp.start()
            three = fut.at[xp, pl.ds(0, 3)]
            spread_all = remote(three, three, f_s, f_r.at[2], col=cols[0])
            spread_all.wait_recv()
            other = to_sib(fut.at[xp], fut.at[xp], f_s, f_r.at[3])
            other.start()
            own.wait_recv()
            other.wait_recv()
            qt = jnp.zeros((emb, n_query), F32)
            for q in range(4):
                ids = lax.broadcasted_iota(jnp.int32, (users, n_query), 0) + q * users
                onehot = jnp.where(ids == qrow[...], 1.0, 0.0).astype(BF16)
                qt = qt + nn(jnp.concatenate([fut[q, k] for k in range(4)], axis=1), onehot)
            q_out[...] = jnp.transpose(qt).astype(BF16)

            @pl.when(r % 2 == 1)
            def _():
                tx_copy(2, J - 1).start()

            three = pl.ds(0, 3)
            to_sib(di.at[three], di_sib.at[three], d_s, d_r.at[0]).wait_send()
            to_xp(di_chip.at[three], di_x.at[three], dx_s, dx_r.at[0]).wait_send()
            to_sib(di.at[three], di_sib.at[three], l_s, d_r.at[0]).wait_send()
            to_sib(fut.at[three], fut.at[three], f_s, f_r.at[0]).wait_send()
        with jax.named_scope('item_finish_2'):
            item_finish(2)
        with jax.named_scope('end'):
            tx_all(2).wait_send()

    dma = pltpu.SemaphoreType.DMA
    scratch = [
        pltpu.VMEM((4, users, quarter), BF16),
        pltpu.VMEM((NSLOT, users, w), jnp.int32),
        pltpu.VMEM((3, 4, emb, quarter), BF16),
        pltpu.VMEM((2, J, emb, w), F32),
        pltpu.VMEM((2, J, emb, w), F32),
        pltpu.VMEM((3, 2, J, emb, w), F32),
        pltpu.VMEM((3, J, emb, w), F32),
        pltpu.VMEM((J, emb, w), F32),
        pltpu.VMEM((emb, users), BF16),
        pltpu.VMEM((4, emb, shard_users), BF16),
        pltpu.VMEM((3, emb, users), F32),
        pltpu.VMEM((3, 4, emb, users), F32),
        pltpu.VMEM((emb, users), F32),
        pltpu.VMEM((users, 128), F32),
        pltpu.VMEM((users, 128), F32),
        pltpu.VMEM((4, J, w), F32),
        pltpu.VMEM((4, J, w), F32),
        pltpu.VMEM((4, J, w), F32),
        pltpu.VMEM((4, J, w), F32),
        pltpu.VMEM((J, w), F32),
        pltpu.VMEM((4, J, w), F32),
        pltpu.VMEM((4, 8, users), F32),
        pltpu.VMEM((users, emb), F32),
        pltpu.VMEM((4, 4, emb, shard_users), BF16),
        pltpu.VMEM((1, n_query), jnp.int32),
        dma((NSLOT,)), dma((2,)), dma((2,)),
        dma, dma((2,)), dma((J,)), dma,
        dma, dma((2, J // 2)),
        dma, dma,
        dma, dma((2, HALF)),
        dma, dma((HALF,)),
        dma, dma((5,)),
        dma, dma((4,)), dma, dma((4,)), dma, dma,
        dma, dma((4,)),
    ]
    vm, hbm = pl.BlockSpec(memory_space=pltpu.VMEM), pl.BlockSpec(memory_space=pltpu.HBM)
    return pl.pallas_call(
        kern,
        out_shape=(jax.ShapeDtypeStruct((emb, shard_users), BF16),
                   jax.ShapeDtypeStruct((J, emb, w), BF16),
                   jax.ShapeDtypeStruct((n_query, emb), BF16)),
        in_specs=[hbm, hbm, hbm, hbm],
        out_specs=(vm, vm, vm),
        scratch_shapes=scratch,
        name='propagate',
        compiler_params=pltpu.CompilerParams(
            collective_id=0, has_side_effects=True, vmem_limit_bytes=VMEM_MIB * 2 ** 20))


def score_kernel(query, fit, fu, scores, item_out, user_out, buf, s_sem, i_sem, u_sem):
    n, _, w = fit.shape
    user_copy = pltpu.make_async_copy(fu, user_out, u_sem)
    user_copy.start()

    def cols(j):
        return pl.ds(pl.multiple_of(j * w, w), w)

    def step(j, carry):
        buf[:, cols(j)] = nn(query[...], fit[j])
        pltpu.make_async_copy(buf.at[:, cols(j)], scores.at[:, cols(j)], s_sem).start()
        pltpu.make_async_copy(fit.at[j], item_out.at[:, cols(j)], i_sem).start()
        return carry

    lax.fori_loop(0, n, step, 0)
    pltpu.make_async_copy(buf, scores, s_sem).wait()
    pltpu.make_async_copy(item_out, item_out, i_sem).wait()
    user_copy.wait()


def score(query, fit, fu):
    n_query, emb = query.shape
    n, _, w = fit.shape
    vm, hbm = pl.BlockSpec(memory_space=pltpu.VMEM), pl.BlockSpec(memory_space=pl.ANY)
    return pl.pallas_call(
        score_kernel,
        out_shape=(jax.ShapeDtypeStruct((n_query, n * w), F32), jax.ShapeDtypeStruct((emb, n * w), BF16),
                   jax.ShapeDtypeStruct(fu.shape, BF16)),
        in_specs=[vm, vm, vm],
        out_specs=(hbm, hbm, hbm),
        scratch_shapes=[pltpu.VMEM((n_query, n * w), F32)] + [pltpu.SemaphoreType.DMA] * 3,
        name='score',
        compiler_params=pltpu.CompilerParams(vmem_limit_bytes=12 * 2 ** 20),
    )(query, fit, fu)


def solution(mesh):
    def device_step(mask_blk, user_shard, item_shard, queries):
        users, width = mask_blk.shape
        quarter, emb = item_shard.shape
        n_query = queries.shape[0]
        call = make_kernel(users, width, quarter, emb, user_shard.shape[0], n_query)
        fu, fit, query = call(*[pltpu.with_memory_space_constraint(a, pltpu.HBM) for a in (
            mask_blk, item_shard.T, user_shard.T, queries.reshape(1, n_query))])
        scores, final_item, final_user = score(query, fit, fu)
        return final_user.T, final_item.T, scores

    return jax.shard_map(device_step, mesh=mesh, in_specs=(P('row', 'col'), P(('row', 'col'), None), P(('col', 'row'), None), P()), out_specs=(P(('row', 'col'), None), P(('col', 'row'), None), P(None, ('col', 'row'))), check_vma=False)
```

```python
import jax
import jax.numpy as jnp
from jax import lax
from jax.experimental import pallas as pl
from jax.experimental.pallas import tpu as pltpu
from jax.sharding import PartitionSpec as P

LAYERS = 3
J = 8
NSLOT = 8
HEAD = 2
NEXT = 5
LEAD = 2
EARLY = 5
FIRST = 5
VMEM_MIB = 52
HALF = 2
F32, BF16 = jnp.float32, jnp.bfloat16


def nt(a, b):
    return lax.dot_general(a, b, (((1,), (1,)), ((), ())), preferred_element_type=F32)


def nn(a, b):
    return lax.dot_general(a, b, (((1,), (0,)), ((), ())), preferred_element_type=F32)


def remote(src, dst, send, recv, **where):
    return pltpu.make_async_remote_copy(
        src_ref=src, dst_ref=dst, send_sem=send, recv_sem=recv,
        device_id=where, device_id_type=pl.DeviceIdType.MESH)


def make_kernel(users, width, quarter, emb, shard_users, n_query):
    w = quarter // J
    piece = quarter // HALF
    rows_blk = 64
    n_rb = users // rows_blk
    lanes = w // 128

    def kern(mask, item, user, queries, fu_out, fit, q_out,
             adj, stage, panel, ps, pk, rs, rx, isum, ut, u0t, usend, urecv, usum,
             rowacc, invu, di, di_sib, di_chip, di_x, di_dg, invi, du, acc, fut, qrow,
             m_sem, i_sem, in_sem, ps_s, ps_r0, ps_r1, ps_rh, tx_s, tx_r, as_s, as_r, ax_s, ax_r, af_s, af_r,
             u_s, u_r, d_s, d_r, dx_s, dx_r, l_s, l_r, f_s, f_r):
        r = lax.axis_index('row')
        c = lax.axis_index('col')
        sib = r + 1 - 2 * (r % 2)
        xp = (r + 2) % 4
        dg = (sib + 2) % 4
        cols = [(c + k) % 4 for k in (1, 2, 3)]

        def over(n, body, start=0):
            def step(j, carry):
                body(j)
                return carry
            lax.fori_loop(start, n, step, 0)

        def part_of(j):
            return pl.ds(pl.multiple_of(j * w, w), w)

        def piece_of(h):
            return pl.ds(pl.multiple_of(h * piece, piece), piece)

        def mask_copy(b):
            return pltpu.make_async_copy(
                mask.at[:, pl.ds(pl.multiple_of(b * w, w), w)], stage.at[b % NSLOT], m_sem.at[b % NSLOT])

        lead = LEAD * w

        def item_copy(k):
            sl = (pl.ds(0, lead), pl.ds(lead, quarter - lead))[k]
            return pltpu.make_async_copy(item.at[:, sl], panel.at[0, r, :, sl], i_sem.at[k])

        for k in range(2):
            item_copy(k).start()
        user_copy = pltpu.make_async_copy(user, u0t.at[c], in_sem.at[0])
        user_copy.start()
        query_copy = pltpu.make_async_copy(queries, qrow, in_sem.at[1])
        query_copy.start()
        for b in range(NSLOT):
            mask_copy(b).start()

        bar = pltpu.get_barrier_semaphore()
        for q in (sib, xp, dg):
            pl.semaphore_signal(bar, inc=1, device_id={'row': q}, device_id_type=pl.DeviceIdType.MESH)
        for q in cols:
            pl.semaphore_signal(bar, inc=1, device_id={'col': q}, device_id_type=pl.DeviceIdType.MESH)

        def to_sib(src, dst, send, recv):
            return remote(src, dst, send, recv, row=sib)

        def to_xp(src, dst, send, recv):
            return remote(src, dst, send, recv, row=xp)

        def ps_near(s, j):
            return to_sib(ps.at[0, j], rs.at[s, 0, j], ps_s, ps_r0.at[s % 2])

        def ps_far(s, j):
            return to_sib(ps.at[1, j], rs.at[s, 1, j], ps_s, ps_r1.at[j])

        def ps_near_all(s):
            return to_sib(ps.at[0], rs.at[s, 0], ps_s, ps_r0.at[s % 2])

        def ps_all(s):
            return to_sib(ps, rs.at[s], ps_s, ps_r0.at[s % 2])

        def tx_copy(s, j):
            return to_xp(pk.at[1, j], rx.at[s, j], tx_s, tx_r.at[s % 2, j // 2])

        def tx_pair(s, i):
            two = pl.ds(2 * i, 2)
            return to_xp(pk.at[1, two], rx.at[s, two], tx_s, tx_r.at[s % 2, i])

        def tx_all(s):
            return to_xp(pk.at[1], rx.at[s], tx_s, tx_r.at[s % 2, 0])

        def as_copy(s, sl, q):
            ref = panel.at[s, q, :, sl]
            return to_sib(ref, ref, as_s, as_r)

        def ax_copy(s, sl, q, h):
            ref = panel.at[s, q, :, sl]
            return to_xp(ref, ref, ax_s, ax_r.at[s % 2, h])

        def af_copy(s, sl, q, h):
            ref = panel.at[s, q, :, sl]
            return to_sib(ref, ref, af_s, af_r.at[h])

        whole = pl.ds(0, quarter)

        def share_far(s, j):
            ax_copy(s, part_of(j), r, j // (J // HALF)).start()

        def share_item(s, j):
            as_copy(s, part_of(j), r).start()
            share_far(s, j)

        def user_copies(kind, src, dst, slot):
            return [remote(src, dst.at[slot], u_s, u_r.at[kind], col=q) for q in cols]

        def user_all(kind, buf):
            three = buf.at[pl.ds(0, 3)]
            return remote(three, three, u_s, u_r.at[kind], col=cols[0])

        def dis_copy(q):
            return to_sib(di.at[q], di_sib.at[q], d_s, d_r.at[q])

        def dix_copy(q):
            return to_xp(di_chip.at[q], di_x.at[q], dx_s, dx_r.at[q])

        def chip_degree(q):
            dis_copy(q).wait_recv()
            di_chip[q] = di[q] + di_sib[q]
            dix_copy(q).start()

        rowacc[...] = jnp.zeros_like(rowacc)

        def mask_pass(q, first=0, last=J):
            def mask_step(j):
                b = q * J + j
                mask_copy(b).wait()
                slot = b % NSLOT

                def rows_step(rb, csum):
                    rows = pl.ds(pl.multiple_of(rb * rows_blk, rows_blk), rows_blk)
                    m = stage[slot, rows, :].astype(F32)
                    adj[q, rows, part_of(j)] = m.astype(BF16)
                    part = m[:, :128]
                    for t in range(1, lanes):
                        part = part + m[:, t * 128:(t + 1) * 128]
                    rowacc[rows, :] = rowacc[rows, :] + part
                    for t in range(0, rows_blk, 8):
                        csum = csum + m[t:t + 8, :]
                    return csum

                csum = lax.fori_loop(0, n_rb, rows_step, jnp.zeros((8, w), F32), unroll=8)
                di[q, pl.ds(j, 1), :] = jnp.sum(csum, axis=0, keepdims=True)

                @pl.when(b + NSLOT < 4 * J)
                def _():
                    mask_copy(b + NSLOT).start()

            over(last, mask_step, first)

        with jax.named_scope('mask_0'):
            mask_pass(0, 0, HEAD)
        with jax.named_scope('first_item'):
            item_copy(0).wait()
            pl.semaphore_wait(bar, 6)
            over(LEAD, lambda j: share_far(0, j))
        with jax.named_scope('mask_0b'):
            mask_pass(0, HEAD, NEXT)
            item_copy(1).wait()
            over(EARLY, lambda j: share_far(0, j), LEAD)
            as_copy(0, whole, r).start()
            user_copy.wait()
            query_copy.wait()
            for cp in user_copies(0, u0t.at[c], u0t, c):
                cp.start()
            mask_pass(0, NEXT)
        dis_copy(0).start()
        for q in range(1, 4):
            with jax.named_scope(f'mask_{q}'):
                mask_pass(q)
            if q < 3:
                dis_copy(q).start()
            chip_degree(q - 1)

        with jax.named_scope('degrees'):
            last_di = [to_sib(di.at[3], di_sib.at[3], l_s, d_r.at[3]), to_xp(di.at[3], di_x.at[3], l_s, dx_r.at[3]),
                       remote(di.at[3], di_dg, l_s, l_r, row=dg)]
            for cp in last_di:
                cp.start()
            over(J, lambda j: share_far(0, j), EARLY)
            user_all(0, u0t).wait_send()
            du[c] = nt(jnp.ones((8, 128), BF16), rowacc[...].astype(BF16))
            for cp in user_copies(4, du.at[c], du, c):
                cp.start()
            user_all(0, u0t).wait_recv()
            u0 = jnp.concatenate([u0t[k] for k in range(4)], axis=1)
            ut[...] = u0
            usum[...] = u0.astype(F32)
            with jax.named_scope('wait_di'):
                for q in range(3):
                    dix_copy(q).wait_recv()
                    invi[q] = lax.rsqrt(jnp.maximum(di_chip[q] + di_x[q], 1.0))
                for cp in last_di:
                    cp.wait_recv()
                invi[3] = lax.rsqrt(jnp.maximum((di[3] + di_sib[3]) + (di_x[3] + di_dg[...]), 1.0))
            with jax.named_scope('wait_du'):
                user_all(4, du).wait_recv()
            deg = ((du[0] + du[1]) + du[2]) + du[3]
            inv_row = lax.rsqrt(jnp.maximum(deg, 1.0))
            invu[...] = jnp.transpose(jnp.broadcast_to(inv_row[0:1, :], (128, users)))

        def form(q, j, off=0, n=w):
            def rows_step(rb, carry):
                rows = pl.ds(pl.multiple_of(rb * rows_blk, rows_blk), rows_blk)
                at = pl.ds(pl.multiple_of(j * w + off, n), n)
                m = adj[q, rows, at].astype(F32)
                iu = jnp.concatenate([invu[rows, :]] * (n // 128), axis=1)
                adj[q, rows, at] = ((iu * m) * invi[q, pl.ds(j, 1), off:off + n]).astype(BF16)
                return carry

            lax.fori_loop(0, n_rb, rows_step, 0, unroll=8)

        def sum_far(s, j):
            ps_far(s, j).wait_recv()
            pk[1, j] = pk[1, j] + rs[s, 1, j]

        def first_part():
            half = w // 2
            sls = [slice(h * half, (h + 1) * half) for h in range(2)]
            ends = [ps_rh, ps_r1.at[0]]

            def half_copy(h):
                return to_sib(ps.at[1, 0, :, sls[h]], rs.at[0, 1, 0, :, sls[h]], ps_s, ends[h])

            for h in range(2):
                form(dg, 0, h * half, half)
                ps[1, 0, :, sls[h]] = nn(ut[...], adj[dg, :, sls[h]])
                half_copy(h).start()
            form(xp, 0)
            pk[1, 0] = nn(ut[...], adj[xp, :, part_of(0)])
            form(sib, 0)
            ps[0, 0] = nn(ut[...], adj[sib, :, part_of(0)])
            ps_near(0, 0).start()
            for h in range(2):
                half_copy(h).wait_recv()
                pk[1, 0, :, sls[h]] = pk[1, 0, :, sls[h]] + rs[0, 1, 0, :, sls[h]]
                to_xp(pk.at[1, 0, :, sls[h]], rx.at[0, 0, :, sls[h]], tx_s, tx_r.at[0, 0]).start()
            form(r, 0)
            pk[0, 0] = nn(ut[...], adj[r, :, part_of(0)])

        def item_part(s):
            def term(q, j):
                if s == 0:
                    form(q, j)
                return nn(ut[...], adj[q, :, part_of(j)])

            def step(j):
                ps[1, j] = term(dg, j)
                ps_far(s, j).start()
                pk[1, j] = term(xp, j)
                ps[0, j] = term(sib, j)
                ps_near(s, j).start()
                pk[0, j] = term(r, j)
                if s == 0:
                    sum_far(s, j)
                    tx_copy(s, j).start()
                elif s == 1:
                    @pl.when(j > 0)
                    def _():
                        sum_far(s, j - 1)
                        tx_copy(s, j - 1).start()
                else:
                    @pl.when(j > 0)
                    def _():
                        sum_far(s, j - 1)

                    @pl.when((j > 0) & (j <= FIRST))
                    def _():
                        tx_copy(s, j - 1).start()

            if s == 0:
                first_part()
            over(J, step, 0 if s else 1)
            if s:
                sum_far(s, J - 1)
            if s == 1:
                tx_copy(s, J - 1).start()

        def item_finish(s):
            ps_near_all(s).wait_recv()

            def finish(j):
                v = ((pk[0, j] + rs[s, 0, j]) + rx[s, j]).astype(BF16)
                before = panel[0, r, :, part_of(j)].astype(F32) if s == 0 else isum[j]
                total = before + v.astype(F32)
                if s < LAYERS - 1:
                    panel[s + 1, r, :, part_of(j)] = v
                    share_item(s + 1, j)
                    isum[j] = total
                else:
                    fit[j] = (total / (LAYERS + 1)).astype(BF16)

            def step(i):
                tx_pair(s, i).wait_recv()
                finish(2 * i)
                finish(2 * i + 1)

            over(J // 2, step)

        def drain(s):
            as_copy(s, whole, r).wait_send()
            ax_copy(s, whole, r, 0).wait_send()

        def user_part(s):
            def add(q, h):
                acc[...] = acc[...] + nt(adj[q, :, piece_of(h)], panel[s, q, :, piece_of(h)])

            acc[...] = jnp.zeros_like(acc)
            over(HALF, lambda h: add(r, h))
            as_copy(s, whole, sib).wait_recv()
            over(HALF, lambda h: add(sib, h))

            def far(h):
                ax_copy(s, piece_of(h), xp, h).wait_recv()
                af_copy(s, piece_of(h), xp, h).start()
                add(xp, h)
                af_copy(s, piece_of(h), dg, h).wait_recv()
                add(dg, h)

            over(HALF, far)
            if s == 0:
                user_all(4, du).wait_send()
            t = jnp.transpose(acc[...])
            usend[s] = t
            urecv[s, c] = t
            for cp in user_copies(s + 1, usend.at[s], urecv.at[s], c):
                cp.start()

        def user_finish(s):
            user_all(s + 1, urecv.at[s]).wait_recv()
            user_all(s + 1, urecv.at[s]).wait_send()
            v = (((urecv[s, 0] + urecv[s, 1]) + urecv[s, 2]) + urecv[s, 3]).astype(BF16)
            ut[...] = v
            usum[...] = usum[...] + v.astype(F32)

        for s in range(LAYERS):
            with jax.named_scope(f'item_part_{s}'):
                item_part(s)
            with jax.named_scope(f'user_part_{s}'):
                user_part(s)
                drain(s)
            if s < LAYERS - 1:
                with jax.named_scope(f'item_finish_{s}'):
                    item_finish(s)
                    tx_all(s).wait_send()
            with jax.named_scope(f'user_finish_{s}'):
                ps_all(s).wait_send()
                af_copy(s, whole, xp, 0).wait_send()
                user_finish(s)

        with jax.named_scope('final_users'):
            fu = (usum[...] / (LAYERS + 1)).astype(BF16)
            for k in range(4):
                fut[r, k] = fu[:, k * shard_users:(k + 1) * shard_users]
            fu_out[...] = fut[r, c]
            cross = to_xp(fut.at[r, c], fut.at[r, c], f_s, f_r.at[0])
            cross.start()
            over(J - 1, lambda j: tx_copy(2, j).start(), FIRST)

            @pl.when(r % 2 == 0)
            def _():
                tx_copy(2, J - 1).start()
            own = to_sib(fut.at[r], fut.at[r], f_s, f_r.at[1])
            own.start()
            cross.wait_recv()
            spread = [remote(fut.at[xp, c], fut.at[xp, c], f_s, f_r.at[2], col=q) for q in cols]
            for cp in spread:
                cp.start()
            three = fut.at[xp, pl.ds(0, 3)]
            spread_all = remote(three, three, f_s, f_r.at[2], col=cols[0])
            spread_all.wait_recv()
            other = to_sib(fut.at[xp], fut.at[xp], f_s, f_r.at[3])
            other.start()
            own.wait_recv()
            other.wait_recv()
            @pl.when(r % 2 == 1)
            def _():
                tx_copy(2, J - 1).start()
            qt = jnp.zeros((emb, n_query), F32)
            for q in range(4):
                ids = lax.broadcasted_iota(jnp.int32, (users, n_query), 0) + q * users
                onehot = jnp.where(ids == qrow[...], 1.0, 0.0).astype(BF16)
                qt = qt + nn(jnp.concatenate([fut[q, k] for k in range(4)], axis=1), onehot)
            q_out[...] = jnp.transpose(qt).astype(BF16)

            three = pl.ds(0, 3)
            to_sib(di.at[three], di_sib.at[three], d_s, d_r.at[0]).wait_send()
            to_xp(di_chip.at[three], di_x.at[three], dx_s, dx_r.at[0]).wait_send()
            to_sib(di.at[three], di_sib.at[three], l_s, d_r.at[0]).wait_send()
            to_sib(fut.at[three], fut.at[three], f_s, f_r.at[0]).wait_send()
        with jax.named_scope('item_finish_2'):
            item_finish(2)
        with jax.named_scope('end'):
            tx_all(2).wait_send()

    dma = pltpu.SemaphoreType.DMA
    scratch = [
        pltpu.VMEM((4, users, quarter), BF16),
        pltpu.VMEM((NSLOT, users, w), jnp.int32),
        pltpu.VMEM((3, 4, emb, quarter), BF16),
        pltpu.VMEM((2, J, emb, w), F32),
        pltpu.VMEM((2, J, emb, w), F32),
        pltpu.VMEM((3, 2, J, emb, w), F32),
        pltpu.VMEM((3, J, emb, w), F32),
        pltpu.VMEM((J, emb, w), F32),
        pltpu.VMEM((emb, users), BF16),
        pltpu.VMEM((4, emb, shard_users), BF16),
        pltpu.VMEM((3, emb, users), F32),
        pltpu.VMEM((3, 4, emb, users), F32),
        pltpu.VMEM((emb, users), F32),
        pltpu.VMEM((users, 128), F32),
        pltpu.VMEM((users, 128), F32),
        pltpu.VMEM((4, J, w), F32),
        pltpu.VMEM((4, J, w), F32),
        pltpu.VMEM((4, J, w), F32),
        pltpu.VMEM((4, J, w), F32),
        pltpu.VMEM((J, w), F32),
        pltpu.VMEM((4, J, w), F32),
        pltpu.VMEM((4, 8, users), F32),
        pltpu.VMEM((users, emb), F32),
        pltpu.VMEM((4, 4, emb, shard_users), BF16),
        pltpu.VMEM((1, n_query), jnp.int32),
        dma((NSLOT,)), dma((2,)), dma((2,)),
        dma, dma((2,)), dma((J,)), dma,
        dma, dma((2, J // 2)),
        dma, dma,
        dma, dma((2, HALF)),
        dma, dma((HALF,)),
        dma, dma((5,)),
        dma, dma((4,)), dma, dma((4,)), dma, dma,
        dma, dma((4,)),
    ]
    vm, hbm = pl.BlockSpec(memory_space=pltpu.VMEM), pl.BlockSpec(memory_space=pltpu.HBM)
    return pl.pallas_call(
        kern,
        out_shape=(jax.ShapeDtypeStruct((emb, shard_users), BF16),
                   jax.ShapeDtypeStruct((J, emb, w), BF16),
                   jax.ShapeDtypeStruct((n_query, emb), BF16)),
        in_specs=[hbm, hbm, hbm, hbm],
        out_specs=(vm, vm, vm),
        scratch_shapes=scratch,
        name='propagate',
        compiler_params=pltpu.CompilerParams(
            collective_id=0, has_side_effects=True, vmem_limit_bytes=VMEM_MIB * 2 ** 20))


def score_kernel(query, fit, fu, scores, item_out, user_out, buf, s_sem, i_sem, u_sem):
    n, _, w = fit.shape
    user_copy = pltpu.make_async_copy(fu, user_out, u_sem)
    user_copy.start()

    def cols(j):
        return pl.ds(pl.multiple_of(j * w, w), w)

    def step(j, carry):
        buf[:, cols(j)] = nn(query[...], fit[j])
        pltpu.make_async_copy(buf.at[:, cols(j)], scores.at[:, cols(j)], s_sem).start()
        pltpu.make_async_copy(fit.at[j], item_out.at[:, cols(j)], i_sem).start()
        return carry

    lax.fori_loop(0, n, step, 0)
    pltpu.make_async_copy(buf, scores, s_sem).wait()
    pltpu.make_async_copy(item_out, item_out, i_sem).wait()
    user_copy.wait()


def score(query, fit, fu):
    n_query, emb = query.shape
    n, _, w = fit.shape
    vm, hbm = pl.BlockSpec(memory_space=pltpu.VMEM), pl.BlockSpec(memory_space=pl.ANY)
    return pl.pallas_call(
        score_kernel,
        out_shape=(jax.ShapeDtypeStruct((n_query, n * w), F32), jax.ShapeDtypeStruct((emb, n * w), BF16),
                   jax.ShapeDtypeStruct(fu.shape, BF16)),
        in_specs=[vm, vm, vm],
        out_specs=(hbm, hbm, hbm),
        scratch_shapes=[pltpu.VMEM((n_query, n * w), F32)] + [pltpu.SemaphoreType.DMA] * 3,
        name='score',
        compiler_params=pltpu.CompilerParams(vmem_limit_bytes=12 * 2 ** 20),
    )(query, fit, fu)


def solution(mesh):
    def device_step(mask_blk, user_shard, item_shard, queries):
        users, width = mask_blk.shape
        quarter, emb = item_shard.shape
        n_query = queries.shape[0]
        call = make_kernel(users, width, quarter, emb, user_shard.shape[0], n_query)
        fu, fit, query = call(*[pltpu.with_memory_space_constraint(a, pltpu.HBM) for a in (
            mask_blk, item_shard.T, user_shard.T, queries.reshape(1, n_query))])
        scores, final_item, final_user = score(query, fit, fu)
        return final_user.T, final_item.T, scores

    return jax.shard_map(device_step, mesh=mesh, in_specs=(P('row', 'col'), P(('row', 'col'), None), P(('col', 'row'), None), P()), out_specs=(P(('row', 'col'), None), P(('col', 'row'), None), P(None, ('col', 'row'))), check_vma=False)
```

```python
import jax
import jax.numpy as jnp
from jax import lax
from jax.experimental import pallas as pl
from jax.experimental.pallas import tpu as pltpu
from jax.sharding import PartitionSpec as P

LAYERS = 3
J = 8
NSLOT = 8
HEAD = 2
NEXT = 5
LEAD = 2
EARLY = 6
FIRST = 5
VMEM_MIB = 52
HALF = 2
F32, BF16 = jnp.float32, jnp.bfloat16


def nt(a, b):
    return lax.dot_general(a, b, (((1,), (1,)), ((), ())), preferred_element_type=F32)


def nn(a, b):
    return lax.dot_general(a, b, (((1,), (0,)), ((), ())), preferred_element_type=F32)


def remote(src, dst, send, recv, **where):
    return pltpu.make_async_remote_copy(
        src_ref=src, dst_ref=dst, send_sem=send, recv_sem=recv,
        device_id=where, device_id_type=pl.DeviceIdType.MESH)


def make_kernel(users, width, quarter, emb, shard_users, n_query):
    w = quarter // J
    piece = quarter // HALF
    rows_blk = 64
    n_rb = users // rows_blk
    lanes = w // 128

    def kern(mask, item, user, queries, fu_out, fit, q_out,
             adj, stage, panel, ps, pk, rs, rx, isum, ut, u0t, usend, urecv, usum,
             rowacc, invu, di, di_sib, di_chip, di_x, di_dg, invi, du, acc, fut, qrow,
             m_sem, i_sem, in_sem, ps_s, ps_r0, ps_r1, ps_rh, tx_s, tx_r, as_s, as_r, ax_s, ax_r, af_s, af_r,
             u_s, u_r, d_s, d_r, dx_s, dx_r, l_s, l_r, f_s, f_r):
        r = lax.axis_index('row')
        c = lax.axis_index('col')
        sib = r + 1 - 2 * (r % 2)
        xp = (r + 2) % 4
        dg = (sib + 2) % 4
        cols = [(c + k) % 4 for k in (1, 2, 3)]

        def over(n, body, start=0):
            def step(j, carry):
                body(j)
                return carry
            lax.fori_loop(start, n, step, 0)

        def part_of(j):
            return pl.ds(pl.multiple_of(j * w, w), w)

        def piece_of(h):
            return pl.ds(pl.multiple_of(h * piece, piece), piece)

        def mask_copy(b):
            return pltpu.make_async_copy(
                mask.at[:, pl.ds(pl.multiple_of(b * w, w), w)], stage.at[b % NSLOT], m_sem.at[b % NSLOT])

        lead = LEAD * w

        def item_copy(k):
            sl = (pl.ds(0, lead), pl.ds(lead, quarter - lead))[k]
            return pltpu.make_async_copy(item.at[:, sl], panel.at[0, r, :, sl], i_sem.at[k])

        for k in range(2):
            item_copy(k).start()
        user_copy = pltpu.make_async_copy(user, u0t.at[c], in_sem.at[0])
        user_copy.start()
        query_copy = pltpu.make_async_copy(queries, qrow, in_sem.at[1])
        query_copy.start()
        for b in range(3):
            mask_copy(b).start()

        bar = pltpu.get_barrier_semaphore()
        for q in (sib, xp, dg):
            pl.semaphore_signal(bar, inc=1, device_id={'row': q}, device_id_type=pl.DeviceIdType.MESH)
        for q in cols:
            pl.semaphore_signal(bar, inc=1, device_id={'col': q}, device_id_type=pl.DeviceIdType.MESH)

        def to_sib(src, dst, send, recv):
            return remote(src, dst, send, recv, row=sib)

        def to_xp(src, dst, send, recv):
            return remote(src, dst, send, recv, row=xp)

        def ps_near(s, j):
            return to_sib(ps.at[0, j], rs.at[s, 0, j], ps_s, ps_r0.at[s % 2])

        def ps_far(s, j):
            return to_sib(ps.at[1, j], rs.at[s, 1, j], ps_s, ps_r1.at[j])

        def ps_near_all(s):
            return to_sib(ps.at[0], rs.at[s, 0], ps_s, ps_r0.at[s % 2])

        def ps_all(s):
            return to_sib(ps, rs.at[s], ps_s, ps_r0.at[s % 2])

        def tx_copy(s, j):
            return to_xp(pk.at[1, j], rx.at[s, j], tx_s, tx_r.at[s % 2, j // 2])

        def tx_pair(s, i):
            two = pl.ds(2 * i, 2)
            return to_xp(pk.at[1, two], rx.at[s, two], tx_s, tx_r.at[s % 2, i])

        def tx_all(s):
            return to_xp(pk.at[1], rx.at[s], tx_s, tx_r.at[s % 2, 0])

        def as_copy(s, sl, q):
            ref = panel.at[s, q, :, sl]
            return to_sib(ref, ref, as_s, as_r)

        def ax_copy(s, sl, q, h):
            ref = panel.at[s, q, :, sl]
            return to_xp(ref, ref, ax_s, ax_r.at[s % 2, h])

        def af_copy(s, sl, q, h):
            ref = panel.at[s, q, :, sl]
            return to_sib(ref, ref, af_s, af_r.at[h])

        whole = pl.ds(0, quarter)

        def share_far(s, j):
            ax_copy(s, part_of(j), r, j // (J // HALF)).start()

        def share_item(s, j):
            as_copy(s, part_of(j), r).start()
            share_far(s, j)

        def user_copies(kind, src, dst, slot):
            return [remote(src, dst.at[slot], u_s, u_r.at[kind], col=q) for q in cols]

        def user_all(kind, buf):
            three = buf.at[pl.ds(0, 3)]
            return remote(three, three, u_s, u_r.at[kind], col=cols[0])

        def dis_copy(q):
            return to_sib(di.at[q], di_sib.at[q], d_s, d_r.at[q])

        def dix_copy(q):
            return to_xp(di_chip.at[q], di_x.at[q], dx_s, dx_r.at[q])

        def chip_degree(q):
            dis_copy(q).wait_recv()
            di_chip[q] = di[q] + di_sib[q]
            dix_copy(q).start()

        rowacc[...] = jnp.zeros_like(rowacc)

        def mask_pass(q, first=0, last=J):
            def mask_step(j):
                b = q * J + j
                mask_copy(b).wait()
                slot = b % NSLOT

                def rows_step(rb, csum):
                    rows = pl.ds(pl.multiple_of(rb * rows_blk, rows_blk), rows_blk)
                    m = stage[slot, rows, :].astype(F32)
                    adj[q, rows, part_of(j)] = m.astype(BF16)
                    part = m[:, :128]
                    for t in range(1, lanes):
                        part = part + m[:, t * 128:(t + 1) * 128]
                    rowacc[rows, :] = rowacc[rows, :] + part
                    for t in range(0, rows_blk, 8):
                        csum = csum + m[t:t + 8, :]
                    return csum

                csum = lax.fori_loop(0, n_rb, rows_step, jnp.zeros((8, w), F32), unroll=8)
                di[q, pl.ds(j, 1), :] = jnp.sum(csum, axis=0, keepdims=True)

                @pl.when(b + NSLOT < 4 * J)
                def _():
                    mask_copy(b + NSLOT).start()

            over(last, mask_step, first)

        for b in range(3, 5):
            mask_copy(b).start()
        with jax.named_scope('mask_0'):
            mask_pass(0, 0, HEAD)
        with jax.named_scope('first_item'):
            item_copy(0).wait()
            for b in range(5, NSLOT):
                mask_copy(b).start()
            pl.semaphore_wait(bar, 6)
            over(LEAD, lambda j: share_far(0, j))
        with jax.named_scope('mask_0b'):
            mask_pass(0, HEAD, NEXT)
            item_copy(1).wait()
            over(EARLY, lambda j: share_far(0, j), LEAD)
            as_copy(0, whole, r).start()
            user_copy.wait()
            query_copy.wait()
            for cp in user_copies(0, u0t.at[c], u0t, c):
                cp.start()
            mask_pass(0, NEXT)
        dis_copy(0).start()
        for q in range(1, 4):
            with jax.named_scope(f'mask_{q}'):
                mask_pass(q, 0, J // 2)
                chip_degree(q - 1)
                mask_pass(q, J // 2)
            if q < 3:
                dis_copy(q).start()

        user_all(0, u0t).wait_send()
        with jax.named_scope('degrees'):
            du[c] = nt(jnp.ones((8, 128), BF16), rowacc[...].astype(BF16))[0:1, :]
            for cp in user_copies(4, du.at[c], du, c):
                cp.start()
            last_di = [to_sib(di.at[3], di_sib.at[3], l_s, d_r.at[3]), to_xp(di.at[3], di_x.at[3], l_s, dx_r.at[3]),
                       remote(di.at[3], di_dg, l_s, l_r, row=dg)]
            for cp in last_di:
                cp.start()
            over(J, lambda j: share_far(0, j), EARLY)
            user_all(0, u0t).wait_recv()
            u0 = jnp.concatenate([u0t[k] for k in range(4)], axis=1)
            ut[...] = u0
            usum[...] = u0.astype(F32)
            with jax.named_scope('wait_di'):
                for q in range(3):
                    dix_copy(q).wait_recv()
                    invi[q] = lax.rsqrt(jnp.maximum(di_chip[q] + di_x[q], 1.0))
                for cp in last_di:
                    cp.wait_recv()
                invi[3] = lax.rsqrt(jnp.maximum((di[3] + di_sib[3]) + (di_x[3] + di_dg[...]), 1.0))
            with jax.named_scope('wait_du'):
                user_all(4, du).wait_recv()
            deg = ((du[0] + du[1]) + du[2]) + du[3]
            inv_row = lax.rsqrt(jnp.maximum(deg, 1.0))
            invu[...] = jnp.transpose(jnp.broadcast_to(inv_row, (128, users)))

        def form(q, j, off=0, n=w):
            def rows_step(rb, carry):
                rows = pl.ds(pl.multiple_of(rb * rows_blk, rows_blk), rows_blk)
                at = pl.ds(pl.multiple_of(j * w + off, n), n)
                m = adj[q, rows, at].astype(F32)
                iu = jnp.concatenate([invu[rows, :]] * (n // 128), axis=1)
                adj[q, rows, at] = ((iu * m) * invi[q, pl.ds(j, 1), off:off + n]).astype(BF16)
                return carry

            lax.fori_loop(0, n_rb, rows_step, 0, unroll=8)

        def sum_far(s, j):
            ps_far(s, j).wait_recv()
            pk[1, j] = pk[1, j] + rs[s, 1, j]

        def first_part():
            half = w // 2
            sls = [slice(h * half, (h + 1) * half) for h in range(2)]
            ends = [ps_rh, ps_r1.at[0]]

            def half_copy(h):
                return to_sib(ps.at[1, 0, :, sls[h]], rs.at[0, 1, 0, :, sls[h]], ps_s, ends[h])

            for h in range(2):
                form(dg, 0, h * half, half)
                ps[1, 0, :, sls[h]] = nn(ut[...], adj[dg, :, sls[h]])
                half_copy(h).start()
            form(xp, 0)
            pk[1, 0] = nn(ut[...], adj[xp, :, part_of(0)])
            form(sib, 0)
            ps[0, 0] = nn(ut[...], adj[sib, :, part_of(0)])
            ps_near(0, 0).start()
            for h in range(2):
                half_copy(h).wait_recv()
                pk[1, 0, :, sls[h]] = pk[1, 0, :, sls[h]] + rs[0, 1, 0, :, sls[h]]
                to_xp(pk.at[1, 0, :, sls[h]], rx.at[0, 0, :, sls[h]], tx_s, tx_r.at[0, 0]).start()
            form(r, 0)
            pk[0, 0] = nn(ut[...], adj[r, :, part_of(0)])

        def item_part(s):
            def term(q, j):
                if s == 0:
                    form(q, j)
                return nn(ut[...], adj[q, :, part_of(j)])

            def step(j):
                ps[1, j] = term(dg, j)
                ps_far(s, j).start()
                pk[1, j] = term(xp, j)
                ps[0, j] = term(sib, j)
                ps_near(s, j).start()
                pk[0, j] = term(r, j)
                if s == 0:
                    sum_far(s, j)
                    tx_copy(s, j).start()
                elif s == 1:
                    @pl.when(j > 0)
                    def _():
                        sum_far(s, j - 1)
                        tx_copy(s, j - 1).start()
                else:
                    @pl.when(j > 0)
                    def _():
                        sum_far(s, j - 1)

                    @pl.when((j > 0) & (j <= FIRST))
                    def _():
                        tx_copy(s, j - 1).start()

            if s == 0:
                first_part()
            over(J, step, 0 if s else 1)
            if s:
                sum_far(s, J - 1)
            if s == 1:
                tx_copy(s, J - 1).start()

        def item_finish(s):
            ps_near_all(s).wait_recv()

            def finish(j):
                v = ((pk[0, j] + rs[s, 0, j]) + rx[s, j]).astype(BF16)
                before = panel[0, r, :, part_of(j)].astype(F32) if s == 0 else isum[j]
                total = before + v.astype(F32)
                if s < LAYERS - 1:
                    panel[s + 1, r, :, part_of(j)] = v
                    share_item(s + 1, j)
                    isum[j] = total
                else:
                    fit[j] = (total / (LAYERS + 1)).astype(BF16)

            def step(i):
                tx_pair(s, i).wait_recv()
                finish(2 * i)
                finish(2 * i + 1)

            over(J // 2, step)

        def drain(s):
            as_copy(s, whole, r).wait_send()
            ax_copy(s, whole, r, 0).wait_send()

        def user_part(s):
            def add(q, h):
                acc[...] = acc[...] + nt(adj[q, :, piece_of(h)], panel[s, q, :, piece_of(h)])

            acc[...] = jnp.zeros_like(acc)
            over(HALF, lambda h: add(r, h))
            as_copy(s, whole, sib).wait_recv()
            over(HALF, lambda h: add(sib, h))

            def far(h):
                ax_copy(s, piece_of(h), xp, h).wait_recv()
                af_copy(s, piece_of(h), xp, h).start()
                add(xp, h)
                af_copy(s, piece_of(h), dg, h).wait_recv()
                add(dg, h)

            over(HALF, far)
            if s == 0:
                user_all(4, du).wait_send()
            t = jnp.transpose(acc[...])
            usend[s] = t
            urecv[s, c] = t
            for cp in user_copies(s + 1, usend.at[s], urecv.at[s], c):
                cp.start()

        def user_finish(s):
            user_all(s + 1, urecv.at[s]).wait_recv()
            user_all(s + 1, urecv.at[s]).wait_send()
            v = (((urecv[s, 0] + urecv[s, 1]) + urecv[s, 2]) + urecv[s, 3]).astype(BF16)
            ut[...] = v
            usum[...] = usum[...] + v.astype(F32)

        for s in range(LAYERS):
            with jax.named_scope(f'item_part_{s}'):
                item_part(s)
            with jax.named_scope(f'user_part_{s}'):
                user_part(s)
                drain(s)
            if s < LAYERS - 1:
                with jax.named_scope(f'item_finish_{s}'):
                    item_finish(s)
                    tx_all(s).wait_send()
            with jax.named_scope(f'user_finish_{s}'):
                ps_all(s).wait_send()
                af_copy(s, whole, xp, 0).wait_send()
                user_finish(s)

        with jax.named_scope('final_users'):
            fu = (usum[...] / (LAYERS + 1)).astype(BF16)
            for k in range(4):
                fut[r, k] = fu[:, k * shard_users:(k + 1) * shard_users]
            fu_out[...] = fut[r, c]
            cross = to_xp(fut.at[r, c], fut.at[r, c], f_s, f_r.at[0])
            cross.start()
            over(J - 1, lambda j: tx_copy(2, j).start(), FIRST)

            @pl.when(r % 2 == 0)
            def _():
                tx_copy(2, J - 1).start()
            own = to_sib(fut.at[r], fut.at[r], f_s, f_r.at[1])
            own.start()
            cross.wait_recv()
            spread = [remote(fut.at[xp, c], fut.at[xp, c], f_s, f_r.at[2], col=q) for q in cols]
            for cp in spread:
                cp.start()
            three = fut.at[xp, pl.ds(0, 3)]
            spread_all = remote(three, three, f_s, f_r.at[2], col=cols[0])
            spread_all.wait_recv()
            other = to_sib(fut.at[xp], fut.at[xp], f_s, f_r.at[3])
            other.start()
            own.wait_recv()
            other.wait_recv()
            @pl.when(r % 2 == 1)
            def _():
                tx_copy(2, J - 1).start()
            qt = jnp.zeros((emb, n_query), F32)
            for q in range(4):
                ids = lax.broadcasted_iota(jnp.int32, (users, n_query), 0) + q * users
                onehot = jnp.where(ids == qrow[...], 1.0, 0.0).astype(BF16)
                qt = qt + nn(jnp.concatenate([fut[q, k] for k in range(4)], axis=1), onehot)
            q_out[...] = jnp.transpose(qt).astype(BF16)

            three = pl.ds(0, 3)
            to_sib(di.at[three], di_sib.at[three], d_s, d_r.at[0]).wait_send()
            to_xp(di_chip.at[three], di_x.at[three], dx_s, dx_r.at[0]).wait_send()
            to_sib(di.at[three], di_sib.at[three], l_s, d_r.at[0]).wait_send()
            to_sib(fut.at[three], fut.at[three], f_s, f_r.at[0]).wait_send()
        with jax.named_scope('item_finish_2'):
            item_finish(2)
        with jax.named_scope('end'):
            tx_all(2).wait_send()

    dma = pltpu.SemaphoreType.DMA
    scratch = [
        pltpu.VMEM((4, users, quarter), BF16),
        pltpu.VMEM((NSLOT, users, w), jnp.int32),
        pltpu.VMEM((3, 4, emb, quarter), BF16),
        pltpu.VMEM((2, J, emb, w), F32),
        pltpu.VMEM((2, J, emb, w), F32),
        pltpu.VMEM((3, 2, J, emb, w), F32),
        pltpu.VMEM((3, J, emb, w), F32),
        pltpu.VMEM((J, emb, w), F32),
        pltpu.VMEM((emb, users), BF16),
        pltpu.VMEM((4, emb, shard_users), BF16),
        pltpu.VMEM((3, emb, users), F32),
        pltpu.VMEM((3, 4, emb, users), F32),
        pltpu.VMEM((emb, users), F32),
        pltpu.VMEM((users, 128), F32),
        pltpu.VMEM((users, 128), F32),
        pltpu.VMEM((4, J, w), F32),
        pltpu.VMEM((4, J, w), F32),
        pltpu.VMEM((4, J, w), F32),
        pltpu.VMEM((4, J, w), F32),
        pltpu.VMEM((J, w), F32),
        pltpu.VMEM((4, J, w), F32),
        pltpu.VMEM((4, 1, users), F32),
        pltpu.VMEM((users, emb), F32),
        pltpu.VMEM((4, 4, emb, shard_users), BF16),
        pltpu.VMEM((1, n_query), jnp.int32),
        dma((NSLOT,)), dma((2,)), dma((2,)),
        dma, dma((2,)), dma((J,)), dma,
        dma, dma((2, J // 2)),
        dma, dma,
        dma, dma((2, HALF)),
        dma, dma((HALF,)),
        dma, dma((5,)),
        dma, dma((4,)), dma, dma((4,)), dma, dma,
        dma, dma((4,)),
    ]
    vm, hbm = pl.BlockSpec(memory_space=pltpu.VMEM), pl.BlockSpec(memory_space=pltpu.HBM)
    return pl.pallas_call(
        kern,
        out_shape=(jax.ShapeDtypeStruct((emb, shard_users), BF16),
                   jax.ShapeDtypeStruct((J, emb, w), BF16),
                   jax.ShapeDtypeStruct((n_query, emb), BF16)),
        in_specs=[hbm, hbm, hbm, hbm],
        out_specs=(vm, vm, vm),
        scratch_shapes=scratch,
        name='propagate',
        compiler_params=pltpu.CompilerParams(
            collective_id=0, has_side_effects=True, vmem_limit_bytes=VMEM_MIB * 2 ** 20))


def score_kernel(query, fit, fu, scores, item_out, user_out, buf, s_sem, i_sem, u_sem):
    n, _, w = fit.shape
    user_copy = pltpu.make_async_copy(fu, user_out, u_sem)
    user_copy.start()

    def cols(j):
        return pl.ds(pl.multiple_of(j * w, w), w)

    def step(j, carry):
        buf[:, cols(j)] = nn(query[...], fit[j])
        pltpu.make_async_copy(buf.at[:, cols(j)], scores.at[:, cols(j)], s_sem).start()
        pltpu.make_async_copy(fit.at[j], item_out.at[:, cols(j)], i_sem).start()
        return carry

    lax.fori_loop(0, n, step, 0)
    pltpu.make_async_copy(buf, scores, s_sem).wait()
    pltpu.make_async_copy(item_out, item_out, i_sem).wait()
    user_copy.wait()


def score(query, fit, fu):
    n_query, emb = query.shape
    n, _, w = fit.shape
    vm, hbm = pl.BlockSpec(memory_space=pltpu.VMEM), pl.BlockSpec(memory_space=pl.ANY)
    return pl.pallas_call(
        score_kernel,
        out_shape=(jax.ShapeDtypeStruct((n_query, n * w), F32), jax.ShapeDtypeStruct((emb, n * w), BF16),
                   jax.ShapeDtypeStruct(fu.shape, BF16)),
        in_specs=[vm, vm, vm],
        out_specs=(hbm, hbm, hbm),
        scratch_shapes=[pltpu.VMEM((n_query, n * w), F32)] + [pltpu.SemaphoreType.DMA] * 3,
        name='score',
        compiler_params=pltpu.CompilerParams(vmem_limit_bytes=12 * 2 ** 20),
    )(query, fit, fu)


def solution(mesh):
    def device_step(mask_blk, user_shard, item_shard, queries):
        users, width = mask_blk.shape
        quarter, emb = item_shard.shape
        n_query = queries.shape[0]
        call = make_kernel(users, width, quarter, emb, user_shard.shape[0], n_query)
        fu, fit, query = call(*[pltpu.with_memory_space_constraint(a, pltpu.HBM) for a in (
            mask_blk, item_shard.T, user_shard.T, queries.reshape(1, n_query))])
        scores, final_item, final_user = score(query, fit, fu)
        return final_user.T, final_item.T, scores

    return jax.shard_map(device_step, mesh=mesh, in_specs=(P('row', 'col'), P(('row', 'col'), None), P(('col', 'row'), None), P()), out_specs=(P(('row', 'col'), None), P(('col', 'row'), None), P(None, ('col', 'row'))), check_vma=False)
```

```python
import jax
import jax.numpy as jnp
from jax import lax
from jax.experimental import pallas as pl
from jax.experimental.pallas import tpu as pltpu
from jax.sharding import PartitionSpec as P

LAYERS = 3
J = 8
NSLOT = 8
HEAD = 2
NEXT = 5
LEAD = 2
EARLY = 6
FIRST = 5
VMEM_MIB = 52
HALF = 2
F32, BF16 = jnp.float32, jnp.bfloat16


def nt(a, b):
    return lax.dot_general(a, b, (((1,), (1,)), ((), ())), preferred_element_type=F32)


def nn(a, b):
    return lax.dot_general(a, b, (((1,), (0,)), ((), ())), preferred_element_type=F32)


def remote(src, dst, send, recv, **where):
    return pltpu.make_async_remote_copy(
        src_ref=src, dst_ref=dst, send_sem=send, recv_sem=recv,
        device_id=where, device_id_type=pl.DeviceIdType.MESH)


def make_kernel(users, width, quarter, emb, shard_users, n_query):
    w = quarter // J
    piece = quarter // HALF
    rows_blk = 64
    n_rb = users // rows_blk
    lanes = w // 128

    def kern(mask, item, user, queries, fu_out, fit, q_out,
             adj, stage, panel, ps, pk, rs, rx, isum, ut, u0t, usend, urecv, usum,
             rowacc, invu, di, di_sib, di_chip, di_x, di_dg, invi, du, acc, fut, qrow,
             m_sib, ut_sib, du_sib, invu_sib,
             m_sem, i_sem, in_sem, ps_s, ps_r0, ps_r1, tx_s, tx_r, as_s, as_r, ax_s, ax_r, af_s, af_r,
             u_s, u_r, d_s, d_r, dx_s, dx_r, l_s, l_r, f_s, f_r,
             sm_s, sm_r, su_s, su_r, sd_s, sd_r):
        r = lax.axis_index('row')
        c = lax.axis_index('col')
        sib = r + 1 - 2 * (r % 2)
        xp = (r + 2) % 4
        dg = (sib + 2) % 4
        cols = [(c + k) % 4 for k in (1, 2, 3)]

        def over(n, body, start=0):
            def step(j, carry):
                body(j)
                return carry
            lax.fori_loop(start, n, step, 0)

        def part_of(j):
            return pl.ds(pl.multiple_of(j * w, w), w)

        def piece_of(h):
            return pl.ds(pl.multiple_of(h * piece, piece), piece)

        def mask_copy(b):
            return pltpu.make_async_copy(
                mask.at[:, pl.ds(pl.multiple_of(b * w, w), w)], stage.at[b % NSLOT], m_sem.at[b % NSLOT])

        lead = LEAD * w

        def item_copy(k):
            sl = (pl.ds(0, lead), pl.ds(lead, quarter - lead))[k]
            return pltpu.make_async_copy(item.at[:, sl], panel.at[0, r, :, sl], i_sem.at[k])

        for k in range(2):
            item_copy(k).start()
        user_copy = pltpu.make_async_copy(user, u0t.at[c], in_sem.at[0])
        user_copy.start()
        query_copy = pltpu.make_async_copy(queries, qrow, in_sem.at[1])
        query_copy.start()
        for b in range(3):
            mask_copy(b).start()

        bar = pltpu.get_barrier_semaphore()
        for q in (sib, xp, dg):
            pl.semaphore_signal(bar, inc=1, device_id={'row': q}, device_id_type=pl.DeviceIdType.MESH)
        for q in cols:
            pl.semaphore_signal(bar, inc=1, device_id={'col': q}, device_id_type=pl.DeviceIdType.MESH)
            pl.semaphore_signal(bar, inc=1, device_id={'row': sib, 'col': q}, device_id_type=pl.DeviceIdType.MESH)

        def to_sib(src, dst, send, recv):
            return remote(src, dst, send, recv, row=sib)

        def to_xp(src, dst, send, recv):
            return remote(src, dst, send, recv, row=xp)

        def ps_near(s, j):
            return to_sib(ps.at[0, j], rs.at[s, 0, j], ps_s, ps_r0.at[s % 2])

        def ps_far(s, j):
            return to_sib(ps.at[1, j], rs.at[s, 1, j], ps_s, ps_r1.at[j])

        def ps_near_all(s):
            return to_sib(ps.at[0], rs.at[s, 0], ps_s, ps_r0.at[s % 2])

        def ps_all(s):
            return to_sib(ps, rs.at[s], ps_s, ps_r0.at[s % 2])

        def tx_copy(s, j):
            return to_xp(pk.at[1, j], rx.at[s, j], tx_s, tx_r.at[s % 2, j // 2])

        def tx_pair(s, i):
            two = pl.ds(2 * i, 2)
            return to_xp(pk.at[1, two], rx.at[s, two], tx_s, tx_r.at[s % 2, i])

        def tx_all(s):
            return to_xp(pk.at[1], rx.at[s], tx_s, tx_r.at[s % 2, 0])

        def as_copy(s, sl, q):
            ref = panel.at[s, q, :, sl]
            return to_sib(ref, ref, as_s, as_r)

        def ax_copy(s, sl, q, h):
            ref = panel.at[s, q, :, sl]
            return to_xp(ref, ref, ax_s, ax_r.at[s % 2, h])

        def af_copy(s, sl, q, h):
            ref = panel.at[s, q, :, sl]
            return to_sib(ref, ref, af_s, af_r.at[h])

        whole = pl.ds(0, quarter)

        def share_far(s, j):
            ax_copy(s, part_of(j), r, j // (J // HALF)).start()

        def share_item(s, j):
            as_copy(s, part_of(j), r).start()
            share_far(s, j)

        def user_copies(kind, src, dst, slot):
            return [remote(src, dst.at[slot], u_s, u_r.at[kind], col=q) for q in cols]

        def user_all(kind, buf):
            three = buf.at[pl.ds(0, 3)]
            return remote(three, three, u_s, u_r.at[kind], col=cols[0])

        def dis_copy(q):
            return to_sib(di.at[q], di_sib.at[q], d_s, d_r.at[q])

        def dix_copy(q):
            return to_xp(di_chip.at[q], di_x.at[q], dx_s, dx_r.at[q])

        def chip_degree(q):
            dis_copy(q).wait_recv()
            di_chip[q] = di[q] + di_sib[q]
            dix_copy(q).start()

        rowacc[...] = jnp.zeros_like(rowacc)

        def mask_pass(q, first=0, last=J):
            def mask_step(j):
                b = q * J + j
                mask_copy(b).wait()
                slot = b % NSLOT

                def rows_step(rb, csum):
                    rows = pl.ds(pl.multiple_of(rb * rows_blk, rows_blk), rows_blk)
                    m = stage[slot, rows, :].astype(F32)
                    adj[q, rows, part_of(j)] = m.astype(BF16)
                    part = m[:, :128]
                    for t in range(1, lanes):
                        part = part + m[:, t * 128:(t + 1) * 128]
                    rowacc[rows, :] = rowacc[rows, :] + part
                    for t in range(0, rows_blk, 8):
                        csum = csum + m[t:t + 8, :]
                    return csum

                csum = lax.fori_loop(0, n_rb, rows_step, jnp.zeros((8, w), F32), unroll=8)
                di[q, pl.ds(j, 1), :] = jnp.sum(csum, axis=0, keepdims=True)

                @pl.when(b + NSLOT < 4 * J)
                def _():
                    mask_copy(b + NSLOT).start()

            over(last, mask_step, first)

        for b in range(3, 5):
            mask_copy(b).start()
        with jax.named_scope('mask_0'):
            mask_pass(0, 0, HEAD)
        with jax.named_scope('first_item'):
            item_copy(0).wait()
            for b in range(5, NSLOT):
                mask_copy(b).start()
            pl.semaphore_wait(bar, 9)
            over(LEAD, lambda j: share_far(0, j))
        with jax.named_scope('mask_0b'):
            mask_pass(0, HEAD, NEXT)
            item_copy(1).wait()
            over(EARLY, lambda j: share_far(0, j), LEAD)
            as_copy(0, whole, r).start()
            user_copy.wait()
            query_copy.wait()
            for cp in user_copies(0, u0t.at[c], u0t, c):
                cp.start()
            mask_pass(0, NEXT)
        dis_copy(0).start()
        for q in range(1, 4):
            with jax.named_scope(f'mask_{q}'):
                mask_pass(q, 0, J // 2)
                chip_degree(q - 1)
                mask_pass(q, J // 2)
            if q < 3:
                dis_copy(q).start()

        user_all(0, u0t).wait_send()
        half = w // 2
        m_copy = to_sib(adj.at[dg, :, pl.ds(0, half)], m_sib, sm_s, sm_r)
        ut_copy = to_sib(ut, ut_sib, su_s, su_r)
        du_all = to_sib(du_sib, du_sib, sd_s, sd_r)
        with jax.named_scope('degrees'):
            du[c] = nt(jnp.ones((8, 128), BF16), rowacc[...].astype(BF16))[0:1, :]
            for cp in user_copies(4, du.at[c], du, c):
                cp.start()
            for q in cols:
                remote(du.at[c], du_sib.at[c], sd_s, sd_r, row=sib, col=q).start()
            to_sib(du.at[c], du_sib.at[c], sd_s, sd_r).start()
            last_di = [to_sib(di.at[3], di_sib.at[3], l_s, d_r.at[3]), to_xp(di.at[3], di_x.at[3], l_s, dx_r.at[3]),
                       remote(di.at[3], di_dg, l_s, l_r, row=dg)]
            for cp in last_di:
                cp.start()
            over(J, lambda j: share_far(0, j), EARLY)
            m_copy.start()
            user_all(0, u0t).wait_recv()
            u0 = jnp.concatenate([u0t[k] for k in range(4)], axis=1)
            ut[...] = u0
            ut_copy.start()
            usum[...] = u0.astype(F32)
            with jax.named_scope('wait_di'):
                for q in range(3):
                    dix_copy(q).wait_recv()
                    invi[q] = lax.rsqrt(jnp.maximum(di_chip[q] + di_x[q], 1.0))
                for cp in last_di:
                    cp.wait_recv()
                invi[3] = lax.rsqrt(jnp.maximum((di[3] + di_sib[3]) + (di_x[3] + di_dg[...]), 1.0))
            with jax.named_scope('wait_du'):
                user_all(4, du).wait_recv()
            def spread_degree(d):
                deg = ((d[0] + d[1]) + d[2]) + d[3]
                return jnp.transpose(jnp.broadcast_to(lax.rsqrt(jnp.maximum(deg, 1.0)), (128, users)))

            invu[...] = spread_degree(du)
            du_all.wait_recv()
            invu_sib[...] = spread_degree(du_sib)
            ut_copy.wait()
            m_copy.wait()

        def form(q, j, off=0, n=w):
            def rows_step(rb, carry):
                rows = pl.ds(pl.multiple_of(rb * rows_blk, rows_blk), rows_blk)
                at = pl.ds(pl.multiple_of(j * w + off, n), n)
                m = adj[q, rows, at].astype(F32)
                iu = jnp.concatenate([invu[rows, :]] * (n // 128), axis=1)
                adj[q, rows, at] = ((iu * m) * invi[q, pl.ds(j, 1), off:off + n]).astype(BF16)
                return carry

            lax.fori_loop(0, n_rb, rows_step, 0, unroll=8)

        def form_sib():
            def rows_step(rb, carry):
                rows = pl.ds(pl.multiple_of(rb * rows_blk, rows_blk), rows_blk)
                m = m_sib[rows, :].astype(F32)
                iu = jnp.concatenate([invu_sib[rows, :]] * (half // 128), axis=1)
                m_sib[rows, :] = ((iu * m) * invi[xp, 0:1, 0:half]).astype(BF16)
                return carry

            lax.fori_loop(0, n_rb, rows_step, 0, unroll=8)

        def sum_far(s, j):
            ps_far(s, j).wait_recv()
            pk[1, j] = pk[1, j] + rs[s, 1, j]

        def first_part():
            lo, hi = slice(0, half), slice(half, w)
            form(xp, 0, 0, half)
            form_sib()
            pk[1, 0, :, lo] = nn(ut[...], adj[xp, :, lo]) + nn(ut_sib[...], m_sib[...])
            to_xp(pk.at[1, 0, :, lo], rx.at[0, 0, :, lo], tx_s, tx_r.at[0, 0]).start()
            form(dg, 0, half, half)
            ps[1, 0, :, hi] = nn(ut[...], adj[dg, :, hi])
            hi_copy = to_sib(ps.at[1, 0, :, hi], rs.at[0, 1, 0, :, hi], ps_s, ps_r1.at[0])
            hi_copy.start()
            form(dg, 0, 0, half)
            form(xp, 0, half, half)
            pk[1, 0, :, hi] = nn(ut[...], adj[xp, :, hi])
            form(sib, 0)
            ps[0, 0] = nn(ut[...], adj[sib, :, part_of(0)])
            ps_near(0, 0).start()
            hi_copy.wait_recv()
            pk[1, 0, :, hi] = pk[1, 0, :, hi] + rs[0, 1, 0, :, hi]
            to_xp(pk.at[1, 0, :, hi], rx.at[0, 0, :, hi], tx_s, tx_r.at[0, 0]).start()
            form(r, 0)
            pk[0, 0] = nn(ut[...], adj[r, :, part_of(0)])

        def item_part(s):
            def term(q, j):
                if s == 0:
                    form(q, j)
                return nn(ut[...], adj[q, :, part_of(j)])

            def step(j):
                ps[1, j] = term(dg, j)
                ps_far(s, j).start()
                pk[1, j] = term(xp, j)
                ps[0, j] = term(sib, j)
                ps_near(s, j).start()
                pk[0, j] = term(r, j)
                if s == 0:
                    sum_far(s, j)
                    tx_copy(s, j).start()
                elif s == 1:
                    @pl.when(j > 0)
                    def _():
                        sum_far(s, j - 1)
                        tx_copy(s, j - 1).start()
                else:
                    @pl.when(j > 0)
                    def _():
                        sum_far(s, j - 1)

                    @pl.when((j > 0) & (j <= FIRST))
                    def _():
                        tx_copy(s, j - 1).start()

            if s == 0:
                first_part()
            over(J, step, 0 if s else 1)
            if s:
                sum_far(s, J - 1)
            if s == 1:
                tx_copy(s, J - 1).start()

        def item_finish(s):
            ps_near_all(s).wait_recv()

            def finish(j):
                v = ((pk[0, j] + rs[s, 0, j]) + rx[s, j]).astype(BF16)
                before = panel[0, r, :, part_of(j)].astype(F32) if s == 0 else isum[j]
                total = before + v.astype(F32)
                if s < LAYERS - 1:
                    panel[s + 1, r, :, part_of(j)] = v
                    share_item(s + 1, j)
                    isum[j] = total
                else:
                    fit[j] = (total / (LAYERS + 1)).astype(BF16)

            def step(i):
                tx_pair(s, i).wait_recv()
                finish(2 * i)
                finish(2 * i + 1)

            over(J // 2, step)

        def drain(s):
            as_copy(s, whole, r).wait_send()
            ax_copy(s, whole, r, 0).wait_send()

        def user_part(s):
            def add(q, h):
                acc[...] = acc[...] + nt(adj[q, :, piece_of(h)], panel[s, q, :, piece_of(h)])

            acc[...] = jnp.zeros_like(acc)
            over(HALF, lambda h: add(r, h))
            as_copy(s, whole, sib).wait_recv()
            over(HALF, lambda h: add(sib, h))

            def far(h):
                ax_copy(s, piece_of(h), xp, h).wait_recv()
                af_copy(s, piece_of(h), xp, h).start()
                add(xp, h)
                af_copy(s, piece_of(h), dg, h).wait_recv()
                add(dg, h)

            over(HALF, far)
            if s == 0:
                user_all(4, du).wait_send()
            t = jnp.transpose(acc[...])
            usend[s] = t
            urecv[s, c] = t
            for cp in user_copies(s + 1, usend.at[s], urecv.at[s], c):
                cp.start()

        def user_finish(s):
            user_all(s + 1, urecv.at[s]).wait_recv()
            user_all(s + 1, urecv.at[s]).wait_send()
            v = (((urecv[s, 0] + urecv[s, 1]) + urecv[s, 2]) + urecv[s, 3]).astype(BF16)
            ut[...] = v
            usum[...] = usum[...] + v.astype(F32)

        for s in range(LAYERS):
            with jax.named_scope(f'item_part_{s}'):
                item_part(s)
            with jax.named_scope(f'user_part_{s}'):
                user_part(s)
                drain(s)
            if s < LAYERS - 1:
                with jax.named_scope(f'item_finish_{s}'):
                    item_finish(s)
                    tx_all(s).wait_send()
            with jax.named_scope(f'user_finish_{s}'):
                if s == 0:
                    to_sib(ps.at[0], rs.at[0, 0], ps_s, ps_r0.at[0]).wait_send()
                    to_sib(ps.at[1, pl.ds(1, J - 1)], rs.at[0, 1, pl.ds(1, J - 1)], ps_s, ps_r0.at[0]).wait_send()
                    to_sib(ps.at[1, 0, :, pl.ds(half, half)], rs.at[0, 1, 0, :, pl.ds(half, half)], ps_s, ps_r0.at[0]).wait_send()
                else:
                    ps_all(s).wait_send()
                af_copy(s, whole, xp, 0).wait_send()
                user_finish(s)

        with jax.named_scope('final_users'):
            fu = (usum[...] / (LAYERS + 1)).astype(BF16)
            for k in range(4):
                fut[r, k] = fu[:, k * shard_users:(k + 1) * shard_users]
            fu_out[...] = fut[r, c]
            cross = to_xp(fut.at[r, c], fut.at[r, c], f_s, f_r.at[0])
            cross.start()
            over(J - 1, lambda j: tx_copy(2, j).start(), FIRST)

            @pl.when(r % 2 == 0)
            def _():
                tx_copy(2, J - 1).start()
            own = to_sib(fut.at[r], fut.at[r], f_s, f_r.at[1])
            own.start()
            cross.wait_recv()
            spread = [remote(fut.at[xp, c], fut.at[xp, c], f_s, f_r.at[2], col=q) for q in cols]
            for cp in spread:
                cp.start()
            three = fut.at[xp, pl.ds(0, 3)]
            spread_all = remote(three, three, f_s, f_r.at[2], col=cols[0])
            spread_all.wait_recv()
            other = to_sib(fut.at[xp], fut.at[xp], f_s, f_r.at[3])
            other.start()
            own.wait_recv()
            other.wait_recv()
            @pl.when(r % 2 == 1)
            def _():
                tx_copy(2, J - 1).start()
            qt = jnp.zeros((emb, n_query), F32)
            for q in range(4):
                ids = lax.broadcasted_iota(jnp.int32, (users, n_query), 0) + q * users
                onehot = jnp.where(ids == qrow[...], 1.0, 0.0).astype(BF16)
                qt = qt + nn(jnp.concatenate([fut[q, k] for k in range(4)], axis=1), onehot)
            q_out[...] = jnp.transpose(qt).astype(BF16)

            three = pl.ds(0, 3)
            to_sib(di.at[three], di_sib.at[three], d_s, d_r.at[0]).wait_send()
            to_xp(di_chip.at[three], di_x.at[three], dx_s, dx_r.at[0]).wait_send()
            to_sib(di.at[three], di_sib.at[three], l_s, d_r.at[0]).wait_send()
            du_all.wait_send()
            to_sib(fut.at[three], fut.at[three], f_s, f_r.at[0]).wait_send()
        with jax.named_scope('item_finish_2'):
            item_finish(2)
        with jax.named_scope('end'):
            tx_all(2).wait_send()

    dma = pltpu.SemaphoreType.DMA
    scratch = [
        pltpu.VMEM((4, users, quarter), BF16),
        pltpu.VMEM((NSLOT, users, w), jnp.int32),
        pltpu.VMEM((3, 4, emb, quarter), BF16),
        pltpu.VMEM((2, J, emb, w), F32),
        pltpu.VMEM((2, J, emb, w), F32),
        pltpu.VMEM((3, 2, J, emb, w), F32),
        pltpu.VMEM((3, J, emb, w), F32),
        pltpu.VMEM((J, emb, w), F32),
        pltpu.VMEM((emb, users), BF16),
        pltpu.VMEM((4, emb, shard_users), BF16),
        pltpu.VMEM((3, emb, users), F32),
        pltpu.VMEM((3, 4, emb, users), F32),
        pltpu.VMEM((emb, users), F32),
        pltpu.VMEM((users, 128), F32),
        pltpu.VMEM((users, 128), F32),
        pltpu.VMEM((4, J, w), F32),
        pltpu.VMEM((4, J, w), F32),
        pltpu.VMEM((4, J, w), F32),
        pltpu.VMEM((4, J, w), F32),
        pltpu.VMEM((J, w), F32),
        pltpu.VMEM((4, J, w), F32),
        pltpu.VMEM((4, 1, users), F32),
        pltpu.VMEM((users, emb), F32),
        pltpu.VMEM((4, 4, emb, shard_users), BF16),
        pltpu.VMEM((1, n_query), jnp.int32),
        pltpu.VMEM((users, w // 2), BF16),
        pltpu.VMEM((emb, users), BF16),
        pltpu.VMEM((4, 1, users), F32),
        pltpu.VMEM((users, 128), F32),
        dma((NSLOT,)), dma((2,)), dma((2,)),
        dma, dma((2,)), dma((J,)),
        dma, dma((2, J // 2)),
        dma, dma,
        dma, dma((2, HALF)),
        dma, dma((HALF,)),
        dma, dma((5,)),
        dma, dma((4,)), dma, dma((4,)), dma, dma,
        dma, dma((4,)),
        dma, dma, dma, dma, dma, dma,
    ]
    vm, hbm = pl.BlockSpec(memory_space=pltpu.VMEM), pl.BlockSpec(memory_space=pltpu.HBM)
    return pl.pallas_call(
        kern,
        out_shape=(jax.ShapeDtypeStruct((emb, shard_users), BF16),
                   jax.ShapeDtypeStruct((J, emb, w), BF16),
                   jax.ShapeDtypeStruct((n_query, emb), BF16)),
        in_specs=[hbm, hbm, hbm, hbm],
        out_specs=(vm, vm, vm),
        scratch_shapes=scratch,
        name='propagate',
        compiler_params=pltpu.CompilerParams(
            collective_id=0, has_side_effects=True, vmem_limit_bytes=VMEM_MIB * 2 ** 20))


def score_kernel(query, fit, fu, scores, item_out, user_out, buf, s_sem, i_sem, u_sem):
    n, _, w = fit.shape
    user_copy = pltpu.make_async_copy(fu, user_out, u_sem)
    user_copy.start()

    def cols(j):
        return pl.ds(pl.multiple_of(j * w, w), w)

    def step(j, carry):
        buf[:, cols(j)] = nn(query[...], fit[j])
        pltpu.make_async_copy(buf.at[:, cols(j)], scores.at[:, cols(j)], s_sem).start()
        pltpu.make_async_copy(fit.at[j], item_out.at[:, cols(j)], i_sem).start()
        return carry

    lax.fori_loop(0, n, step, 0)
    pltpu.make_async_copy(buf, scores, s_sem).wait()
    pltpu.make_async_copy(item_out, item_out, i_sem).wait()
    user_copy.wait()


def score(query, fit, fu):
    n_query, emb = query.shape
    n, _, w = fit.shape
    vm, hbm = pl.BlockSpec(memory_space=pltpu.VMEM), pl.BlockSpec(memory_space=pl.ANY)
    return pl.pallas_call(
        score_kernel,
        out_shape=(jax.ShapeDtypeStruct((n_query, n * w), F32), jax.ShapeDtypeStruct((emb, n * w), BF16),
                   jax.ShapeDtypeStruct(fu.shape, BF16)),
        in_specs=[vm, vm, vm],
        out_specs=(hbm, hbm, hbm),
        scratch_shapes=[pltpu.VMEM((n_query, n * w), F32)] + [pltpu.SemaphoreType.DMA] * 3,
        name='score',
        compiler_params=pltpu.CompilerParams(vmem_limit_bytes=12 * 2 ** 20),
    )(query, fit, fu)


def solution(mesh):
    def device_step(mask_blk, user_shard, item_shard, queries):
        users, width = mask_blk.shape
        quarter, emb = item_shard.shape
        n_query = queries.shape[0]
        call = make_kernel(users, width, quarter, emb, user_shard.shape[0], n_query)
        fu, fit, query = call(*[pltpu.with_memory_space_constraint(a, pltpu.HBM) for a in (
            mask_blk, item_shard.T, user_shard.T, queries.reshape(1, n_query))])
        scores, final_item, final_user = score(query, fit, fu)
        return final_user.T, final_item.T, scores

    return jax.shard_map(device_step, mesh=mesh, in_specs=(P('row', 'col'), P(('row', 'col'), None), P(('col', 'row'), None), P()), out_specs=(P(('row', 'col'), None), P(('col', 'row'), None), P(None, ('col', 'row'))), check_vma=False)
```

```python
import jax
import jax.numpy as jnp
from jax import lax
from jax.experimental import pallas as pl
from jax.experimental.pallas import tpu as pltpu
from jax.sharding import PartitionSpec as P

LAYERS = 3
J = 8
NSLOT = 8
HEAD = 2
NEXT = 5
LEAD = 2
EARLY = 6
FIRST = 5
VMEM_MIB = 52
HALF = 2
F32, BF16 = jnp.float32, jnp.bfloat16


def nt(a, b):
    return lax.dot_general(a, b, (((1,), (1,)), ((), ())), preferred_element_type=F32)


def nn(a, b):
    return lax.dot_general(a, b, (((1,), (0,)), ((), ())), preferred_element_type=F32)


def remote(src, dst, send, recv, **where):
    return pltpu.make_async_remote_copy(
        src_ref=src, dst_ref=dst, send_sem=send, recv_sem=recv,
        device_id=where, device_id_type=pl.DeviceIdType.MESH)


def make_kernel(users, width, quarter, emb, shard_users, n_query):
    w = quarter // J
    piece = quarter // HALF
    rows_blk = 64
    n_rb = users // rows_blk
    lanes = w // 128

    def kern(mask, item, user, queries, fu_out, fit, q_out,
             adj, stage, panel, ps, pk, rs, rx, isum, ut, u0t, usend, urecv, usum,
             rowacc, invu, di, di_sib, di_chip, di_x, di_dg, invi, du, acc, fut, qrow,
             m_sib, ut_sib, du_sib, invu_sib, qacc,
             m_sem, i_sem, in_sem, ps_s, ps_r0, ps_r1, tx_s, tx_r, as_s, as_r, ax_s, ax_r, af_s, af_r,
             u_s, u_r, d_s, d_r, dx_s, dx_r, l_s, l_r, f_s, f_r,
             sm_s, sm_r, su_s, su_r, sd_s, sd_r):
        r = lax.axis_index('row')
        c = lax.axis_index('col')
        sib = r + 1 - 2 * (r % 2)
        xp = (r + 2) % 4
        dg = (sib + 2) % 4
        cols = [(c + k) % 4 for k in (1, 2, 3)]

        def over(n, body, start=0):
            def step(j, carry):
                body(j)
                return carry
            lax.fori_loop(start, n, step, 0)

        def part_of(j):
            return pl.ds(pl.multiple_of(j * w, w), w)

        def piece_of(h):
            return pl.ds(pl.multiple_of(h * piece, piece), piece)

        def mask_copy(b):
            return pltpu.make_async_copy(
                mask.at[:, pl.ds(pl.multiple_of(b * w, w), w)], stage.at[b % NSLOT], m_sem.at[b % NSLOT])

        lead = LEAD * w

        def item_copy(k):
            sl = (pl.ds(0, lead), pl.ds(lead, quarter - lead))[k]
            return pltpu.make_async_copy(item.at[:, sl], panel.at[0, r, :, sl], i_sem.at[k])

        for k in range(2):
            item_copy(k).start()
        user_copy = pltpu.make_async_copy(user, u0t.at[c], in_sem.at[0])
        user_copy.start()
        query_copy = pltpu.make_async_copy(queries, qrow, in_sem.at[1])
        query_copy.start()
        for b in range(3):
            mask_copy(b).start()

        bar = pltpu.get_barrier_semaphore()
        for q in (sib, xp, dg):
            pl.semaphore_signal(bar, inc=1, device_id={'row': q}, device_id_type=pl.DeviceIdType.MESH)
        for q in cols:
            pl.semaphore_signal(bar, inc=1, device_id={'col': q}, device_id_type=pl.DeviceIdType.MESH)
            pl.semaphore_signal(bar, inc=1, device_id={'row': sib, 'col': q}, device_id_type=pl.DeviceIdType.MESH)

        def to_sib(src, dst, send, recv):
            return remote(src, dst, send, recv, row=sib)

        def to_xp(src, dst, send, recv):
            return remote(src, dst, send, recv, row=xp)

        def ps_near(s, j):
            return to_sib(ps.at[0, j], rs.at[s, 0, j], ps_s, ps_r0.at[s % 2])

        def ps_far(s, j):
            return to_sib(ps.at[1, j], rs.at[s, 1, j], ps_s, ps_r1.at[j])

        def ps_near_all(s):
            return to_sib(ps.at[0], rs.at[s, 0], ps_s, ps_r0.at[s % 2])

        def ps_all(s):
            return to_sib(ps, rs.at[s], ps_s, ps_r0.at[s % 2])

        def tx_copy(s, j):
            return to_xp(pk.at[1, j], rx.at[s, j], tx_s, tx_r.at[s % 2, j // 2])

        def tx_pair(s, i):
            two = pl.ds(2 * i, 2)
            return to_xp(pk.at[1, two], rx.at[s, two], tx_s, tx_r.at[s % 2, i])

        def tx_all(s):
            return to_xp(pk.at[1], rx.at[s], tx_s, tx_r.at[s % 2, 0])

        def as_copy(s, sl, q):
            ref = panel.at[s, q, :, sl]
            return to_sib(ref, ref, as_s, as_r)

        def ax_copy(s, sl, q, h):
            ref = panel.at[s, q, :, sl]
            return to_xp(ref, ref, ax_s, ax_r.at[s % 2, h])

        def af_copy(s, sl, q, h):
            ref = panel.at[s, q, :, sl]
            return to_sib(ref, ref, af_s, af_r.at[h])

        whole = pl.ds(0, quarter)

        def share_far(s, j):
            ax_copy(s, part_of(j), r, j // (J // HALF)).start()

        def share_item(s, j):
            as_copy(s, part_of(j), r).start()
            share_far(s, j)

        def user_copies(kind, src, dst, slot):
            return [remote(src, dst.at[slot], u_s, u_r.at[kind], col=q) for q in cols]

        def user_all(kind, buf):
            three = buf.at[pl.ds(0, 3)]
            return remote(three, three, u_s, u_r.at[kind], col=cols[0])

        def dis_copy(q):
            return to_sib(di.at[q], di_sib.at[q], d_s, d_r.at[q])

        def dix_copy(q):
            return to_xp(di_chip.at[q], di_x.at[q], dx_s, dx_r.at[q])

        def chip_degree(q):
            dis_copy(q).wait_recv()
            di_chip[q] = di[q] + di_sib[q]
            dix_copy(q).start()

        rowacc[...] = jnp.zeros_like(rowacc)

        def mask_pass(q, first=0, last=J):
            def mask_step(j):
                b = q * J + j
                mask_copy(b).wait()
                slot = b % NSLOT

                def rows_step(rb, csum):
                    rows = pl.ds(pl.multiple_of(rb * rows_blk, rows_blk), rows_blk)
                    m = stage[slot, rows, :].astype(F32)
                    adj[q, rows, part_of(j)] = m.astype(BF16)
                    part = m[:, :128]
                    for t in range(1, lanes):
                        part = part + m[:, t * 128:(t + 1) * 128]
                    rowacc[rows, :] = rowacc[rows, :] + part
                    for t in range(0, rows_blk, 8):
                        csum = csum + m[t:t + 8, :]
                    return csum

                csum = lax.fori_loop(0, n_rb, rows_step, jnp.zeros((8, w), F32), unroll=8)
                di[q, pl.ds(j, 1), :] = jnp.sum(csum, axis=0, keepdims=True)

                @pl.when(b + NSLOT < 4 * J)
                def _():
                    mask_copy(b + NSLOT).start()

            over(last, mask_step, first)

        for b in range(3, 5):
            mask_copy(b).start()
        with jax.named_scope('mask_0'):
            mask_pass(0, 0, HEAD)
        with jax.named_scope('first_item'):
            item_copy(0).wait()
            for b in range(5, NSLOT):
                mask_copy(b).start()
            pl.semaphore_wait(bar, 9)
            over(LEAD, lambda j: share_far(0, j))
        with jax.named_scope('mask_0b'):
            mask_pass(0, HEAD, NEXT)
            item_copy(1).wait()
            over(EARLY, lambda j: share_far(0, j), LEAD)
            as_copy(0, whole, r).start()
            user_copy.wait()
            query_copy.wait()
            for cp in user_copies(0, u0t.at[c], u0t, c):
                cp.start()
            mask_pass(0, NEXT)
        dis_copy(0).start()
        half = w // 2
        m_copy = to_sib(adj.at[dg, :, pl.ds(0, half)], m_sib, sm_s, sm_r)
        ut_copy = to_sib(ut, ut_sib, su_s, su_r)
        du_all = to_sib(du_sib, du_sib, sd_s, sd_r)
        for q in range(1, 4):
            with jax.named_scope(f'mask_{q}'):
                mask_pass(q, 0, J // 2)
                chip_degree(q - 1)
                if q == 3:
                    m_copy.start()
                    user_all(0, u0t).wait_recv()
                    user_all(0, u0t).wait_send()
                    u0 = jnp.concatenate([u0t[k] for k in range(4)], axis=1)
                    ut[...] = u0
                    ut_copy.start()
                    usum[...] = u0.astype(F32)
                mask_pass(q, J // 2)
            if q < 3:
                dis_copy(q).start()

        with jax.named_scope('degrees'):
            du[c] = nt(jnp.ones((8, 128), BF16), rowacc[...].astype(BF16))[0:1, :]
            for cp in user_copies(4, du.at[c], du, c):
                cp.start()
            for q in cols:
                remote(du.at[c], du_sib.at[c], sd_s, sd_r, row=sib, col=q).start()
            to_sib(du.at[c], du_sib.at[c], sd_s, sd_r).start()
            last_di = [to_sib(di.at[3], di_sib.at[3], l_s, d_r.at[3]), to_xp(di.at[3], di_x.at[3], l_s, dx_r.at[3]),
                       remote(di.at[3], di_dg, l_s, l_r, row=dg)]
            for cp in last_di:
                cp.start()
            over(J, lambda j: share_far(0, j), EARLY)
            with jax.named_scope('wait_di'):
                for q in range(3):
                    dix_copy(q).wait_recv()
                    invi[q] = lax.rsqrt(jnp.maximum(di_chip[q] + di_x[q], 1.0))
                for cp in last_di:
                    cp.wait_recv()
                invi[3] = lax.rsqrt(jnp.maximum((di[3] + di_sib[3]) + (di_x[3] + di_dg[...]), 1.0))
            with jax.named_scope('wait_du'):
                user_all(4, du).wait_recv()
            def spread_degree(d):
                deg = ((d[0] + d[1]) + d[2]) + d[3]
                return jnp.transpose(jnp.broadcast_to(lax.rsqrt(jnp.maximum(deg, 1.0)), (128, users)))

            invu[...] = spread_degree(du)
            du_all.wait_recv()
            invu_sib[...] = spread_degree(du_sib)
            ut_copy.wait()
            m_copy.wait()

        def form(q, j, off=0, n=w):
            def rows_step(rb, carry):
                rows = pl.ds(pl.multiple_of(rb * rows_blk, rows_blk), rows_blk)
                at = pl.ds(pl.multiple_of(j * w + off, n), n)
                m = adj[q, rows, at].astype(F32)
                iu = jnp.concatenate([invu[rows, :]] * (n // 128), axis=1)
                adj[q, rows, at] = ((iu * m) * invi[q, pl.ds(j, 1), off:off + n]).astype(BF16)
                return carry

            lax.fori_loop(0, n_rb, rows_step, 0, unroll=8)

        def form_sib():
            def rows_step(rb, carry):
                rows = pl.ds(pl.multiple_of(rb * rows_blk, rows_blk), rows_blk)
                m = m_sib[rows, :].astype(F32)
                iu = jnp.concatenate([invu_sib[rows, :]] * (half // 128), axis=1)
                m_sib[rows, :] = ((iu * m) * invi[xp, 0:1, 0:half]).astype(BF16)
                return carry

            lax.fori_loop(0, n_rb, rows_step, 0, unroll=8)

        def sum_far(s, j):
            ps_far(s, j).wait_recv()
            pk[1, j] = pk[1, j] + rs[s, 1, j]

        def first_part():
            lo, hi = slice(0, half), slice(half, w)
            form(xp, 0, 0, half)
            form_sib()
            pk[1, 0, :, lo] = nn(ut[...], adj[xp, :, lo]) + nn(ut_sib[...], m_sib[...])
            to_xp(pk.at[1, 0, :, lo], rx.at[0, 0, :, lo], tx_s, tx_r.at[0, 0]).start()
            form(dg, 0, half, half)
            ps[1, 0, :, hi] = nn(ut[...], adj[dg, :, hi])
            hi_copy = to_sib(ps.at[1, 0, :, hi], rs.at[0, 1, 0, :, hi], ps_s, ps_r1.at[0])
            hi_copy.start()
            form(dg, 0, 0, half)
            form(xp, 0, half, half)
            pk[1, 0, :, hi] = nn(ut[...], adj[xp, :, hi])
            form(sib, 0)
            ps[0, 0] = nn(ut[...], adj[sib, :, part_of(0)])
            ps_near(0, 0).start()
            hi_copy.wait_recv()
            pk[1, 0, :, hi] = pk[1, 0, :, hi] + rs[0, 1, 0, :, hi]
            to_xp(pk.at[1, 0, :, hi], rx.at[0, 0, :, hi], tx_s, tx_r.at[0, 0]).start()
            form(r, 0)
            pk[0, 0] = nn(ut[...], adj[r, :, part_of(0)])

        def item_part(s):
            def term(q, j):
                if s == 0:
                    form(q, j)
                return nn(ut[...], adj[q, :, part_of(j)])

            def step(j):
                ps[1, j] = term(dg, j)
                ps_far(s, j).start()
                pk[1, j] = term(xp, j)
                ps[0, j] = term(sib, j)
                ps_near(s, j).start()
                pk[0, j] = term(r, j)
                if s == 0:
                    sum_far(s, j)
                    tx_copy(s, j).start()
                elif s == 1:
                    @pl.when(j > 0)
                    def _():
                        sum_far(s, j - 1)
                        tx_copy(s, j - 1).start()
                else:
                    @pl.when(j > 0)
                    def _():
                        sum_far(s, j - 1)

                    @pl.when((j > 0) & (j <= FIRST))
                    def _():
                        tx_copy(s, j - 1).start()

            if s == 0:
                first_part()
            over(J, step, 0 if s else 1)
            if s:
                sum_far(s, J - 1)
            if s == 1:
                tx_copy(s, J - 1).start()

        def item_finish(s):
            ps_near_all(s).wait_recv()

            def finish(j):
                v = ((pk[0, j] + rs[s, 0, j]) + rx[s, j]).astype(BF16)
                before = panel[0, r, :, part_of(j)].astype(F32) if s == 0 else isum[j]
                total = before + v.astype(F32)
                if s < LAYERS - 1:
                    panel[s + 1, r, :, part_of(j)] = v
                    share_item(s + 1, j)
                    isum[j] = total
                else:
                    fit[j] = (total / (LAYERS + 1)).astype(BF16)

            def step(i):
                tx_pair(s, i).wait_recv()
                finish(2 * i)
                finish(2 * i + 1)

            over(J // 2, step)

        def drain(s):
            as_copy(s, whole, r).wait_send()
            ax_copy(s, whole, r, 0).wait_send()

        def user_part(s):
            def add(q, h):
                acc[...] = acc[...] + nt(adj[q, :, piece_of(h)], panel[s, q, :, piece_of(h)])

            acc[...] = jnp.zeros_like(acc)
            over(HALF, lambda h: add(r, h))
            as_copy(s, whole, sib).wait_recv()
            over(HALF, lambda h: add(sib, h))

            def far(h):
                ax_copy(s, piece_of(h), xp, h).wait_recv()
                af_copy(s, piece_of(h), xp, h).start()
                add(xp, h)
                af_copy(s, piece_of(h), dg, h).wait_recv()
                add(dg, h)

            over(HALF, far)
            if s == 0:
                user_all(4, du).wait_send()
            t = jnp.transpose(acc[...])
            usend[s] = t
            urecv[s, c] = t
            for cp in user_copies(s + 1, usend.at[s], urecv.at[s], c):
                cp.start()

        def user_finish(s):
            user_all(s + 1, urecv.at[s]).wait_recv()
            user_all(s + 1, urecv.at[s]).wait_send()
            v = (((urecv[s, 0] + urecv[s, 1]) + urecv[s, 2]) + urecv[s, 3]).astype(BF16)
            ut[...] = v
            usum[...] = usum[...] + v.astype(F32)

        for s in range(LAYERS):
            with jax.named_scope(f'item_part_{s}'):
                item_part(s)
            with jax.named_scope(f'user_part_{s}'):
                user_part(s)
                drain(s)
            if s < LAYERS - 1:
                with jax.named_scope(f'item_finish_{s}'):
                    item_finish(s)
                    tx_all(s).wait_send()
            with jax.named_scope(f'user_finish_{s}'):
                if s == 0:
                    to_sib(ps.at[0], rs.at[0, 0], ps_s, ps_r0.at[0]).wait_send()
                    to_sib(ps.at[1, pl.ds(1, J - 1)], rs.at[0, 1, pl.ds(1, J - 1)], ps_s, ps_r0.at[0]).wait_send()
                    to_sib(ps.at[1, 0, :, pl.ds(half, half)], rs.at[0, 1, 0, :, pl.ds(half, half)], ps_s, ps_r0.at[0]).wait_send()
                else:
                    ps_all(s).wait_send()
                af_copy(s, whole, xp, 0).wait_send()
                user_finish(s)

        with jax.named_scope('final_users'):
            fu = (usum[...] / (LAYERS + 1)).astype(BF16)
            for k in range(4):
                fut[r, k] = fu[:, k * shard_users:(k + 1) * shard_users]
            fu_out[...] = fut[r, c]
            cross = to_xp(fut.at[r, c], fut.at[r, c], f_s, f_r.at[0])
            cross.start()
            over(J - 1, lambda j: tx_copy(2, j).start(), FIRST)

            @pl.when(r % 2 == 0)
            def _():
                tx_copy(2, J - 1).start()
            own = to_sib(fut.at[r], fut.at[r], f_s, f_r.at[1])
            own.start()
            cross.wait_recv()
            spread = [remote(fut.at[xp, c], fut.at[xp, c], f_s, f_r.at[2], col=q) for q in cols]
            for cp in spread:
                cp.start()
            three = fut.at[xp, pl.ds(0, 3)]
            spread_all = remote(three, three, f_s, f_r.at[2], col=cols[0])
            spread_all.wait_recv()
            other = to_sib(fut.at[xp], fut.at[xp], f_s, f_r.at[3])
            other.start()
            own.wait_recv()

            def pick(q):
                ids = lax.broadcasted_iota(jnp.int32, (users, n_query), 0) + q * users
                onehot = jnp.where(ids == qrow[...], 1.0, 0.0).astype(BF16)
                return nn(jnp.concatenate([fut[q, k] for k in range(4)], axis=1), onehot)

            qacc[...] = (pick(r) + pick(sib)) + pick(xp)

            other.wait_recv()
            @pl.when(r % 2 == 1)
            def _():
                tx_copy(2, J - 1).start()

            q_out[...] = jnp.transpose(qacc[...] + pick(dg)).astype(BF16)

            three = pl.ds(0, 3)
            to_sib(di.at[three], di_sib.at[three], d_s, d_r.at[0]).wait_send()
            to_xp(di_chip.at[three], di_x.at[three], dx_s, dx_r.at[0]).wait_send()
            to_sib(di.at[three], di_sib.at[three], l_s, d_r.at[0]).wait_send()
            du_all.wait_send()
            to_sib(fut.at[three], fut.at[three], f_s, f_r.at[0]).wait_send()
        with jax.named_scope('item_finish_2'):
            item_finish(2)
        with jax.named_scope('end'):
            tx_all(2).wait_send()

    dma = pltpu.SemaphoreType.DMA
    scratch = [
        pltpu.VMEM((4, users, quarter), BF16),
        pltpu.VMEM((NSLOT, users, w), jnp.int32),
        pltpu.VMEM((3, 4, emb, quarter), BF16),
        pltpu.VMEM((2, J, emb, w), F32),
        pltpu.VMEM((2, J, emb, w), F32),
        pltpu.VMEM((3, 2, J, emb, w), F32),
        pltpu.VMEM((3, J, emb, w), F32),
        pltpu.VMEM((J, emb, w), F32),
        pltpu.VMEM((emb, users), BF16),
        pltpu.VMEM((4, emb, shard_users), BF16),
        pltpu.VMEM((3, emb, users), F32),
        pltpu.VMEM((3, 4, emb, users), F32),
        pltpu.VMEM((emb, users), F32),
        pltpu.VMEM((users, 128), F32),
        pltpu.VMEM((users, 128), F32),
        pltpu.VMEM((4, J, w), F32),
        pltpu.VMEM((4, J, w), F32),
        pltpu.VMEM((4, J, w), F32),
        pltpu.VMEM((4, J, w), F32),
        pltpu.VMEM((J, w), F32),
        pltpu.VMEM((4, J, w), F32),
        pltpu.VMEM((4, 1, users), F32),
        pltpu.VMEM((users, emb), F32),
        pltpu.VMEM((4, 4, emb, shard_users), BF16),
        pltpu.VMEM((1, n_query), jnp.int32),
        pltpu.VMEM((users, w // 2), BF16),
        pltpu.VMEM((emb, users), BF16),
        pltpu.VMEM((4, 1, users), F32),
        pltpu.VMEM((users, 128), F32),
        pltpu.VMEM((emb, n_query), F32),
        dma((NSLOT,)), dma((2,)), dma((2,)),
        dma, dma((2,)), dma((J,)),
        dma, dma((2, J // 2)),
        dma, dma,
        dma, dma((2, HALF)),
        dma, dma((HALF,)),
        dma, dma((5,)),
        dma, dma((4,)), dma, dma((4,)), dma, dma,
        dma, dma((4,)),
        dma, dma, dma, dma, dma, dma,
    ]
    vm, hbm = pl.BlockSpec(memory_space=pltpu.VMEM), pl.BlockSpec(memory_space=pltpu.HBM)
    return pl.pallas_call(
        kern,
        out_shape=(jax.ShapeDtypeStruct((emb, shard_users), BF16),
                   jax.ShapeDtypeStruct((J, emb, w), BF16),
                   jax.ShapeDtypeStruct((n_query, emb), BF16)),
        in_specs=[hbm, hbm, hbm, hbm],
        out_specs=(vm, vm, vm),
        scratch_shapes=scratch,
        name='propagate',
        compiler_params=pltpu.CompilerParams(
            collective_id=0, has_side_effects=True, vmem_limit_bytes=VMEM_MIB * 2 ** 20))


def score_kernel(query, fit, fu, scores, item_out, user_out, buf, s_sem, i_sem, u_sem):
    n, _, w = fit.shape
    user_copy = pltpu.make_async_copy(fu, user_out, u_sem)
    user_copy.start()

    def cols(j):
        return pl.ds(pl.multiple_of(j * w, w), w)

    def step(j, carry):
        buf[:, cols(j)] = nn(query[...], fit[j])
        pltpu.make_async_copy(buf.at[:, cols(j)], scores.at[:, cols(j)], s_sem).start()
        pltpu.make_async_copy(fit.at[j], item_out.at[:, cols(j)], i_sem).start()
        return carry

    lax.fori_loop(0, n, step, 0)
    pltpu.make_async_copy(buf, scores, s_sem).wait()
    pltpu.make_async_copy(item_out, item_out, i_sem).wait()
    user_copy.wait()


def score(query, fit, fu):
    n_query, emb = query.shape
    n, _, w = fit.shape
    vm, hbm = pl.BlockSpec(memory_space=pltpu.VMEM), pl.BlockSpec(memory_space=pl.ANY)
    return pl.pallas_call(
        score_kernel,
        out_shape=(jax.ShapeDtypeStruct((n_query, n * w), F32), jax.ShapeDtypeStruct((emb, n * w), BF16),
                   jax.ShapeDtypeStruct(fu.shape, BF16)),
        in_specs=[vm, vm, vm],
        out_specs=(hbm, hbm, hbm),
        scratch_shapes=[pltpu.VMEM((n_query, n * w), F32)] + [pltpu.SemaphoreType.DMA] * 3,
        name='score',
        compiler_params=pltpu.CompilerParams(vmem_limit_bytes=12 * 2 ** 20),
    )(query, fit, fu)


def solution(mesh):
    def device_step(mask_blk, user_shard, item_shard, queries):
        users, width = mask_blk.shape
        quarter, emb = item_shard.shape
        n_query = queries.shape[0]
        call = make_kernel(users, width, quarter, emb, user_shard.shape[0], n_query)
        fu, fit, query = call(*[pltpu.with_memory_space_constraint(a, pltpu.HBM) for a in (
            mask_blk, item_shard.T, user_shard.T, queries.reshape(1, n_query))])
        scores, final_item, final_user = score(query, fit, fu)
        return final_user.T, final_item.T, scores

    return jax.shard_map(device_step, mesh=mesh, in_specs=(P('row', 'col'), P(('row', 'col'), None), P(('col', 'row'), None), P()), out_specs=(P(('row', 'col'), None), P(('col', 'row'), None), P(None, ('col', 'row'))), check_vma=False)
```

```python
import jax
import jax.numpy as jnp
from jax import lax
from jax.experimental import pallas as pl
from jax.experimental.pallas import tpu as pltpu
from jax.sharding import PartitionSpec as P

LAYERS = 3
J = 8
NSLOT = 8
HEAD = 2
NEXT = 5
LEAD = 2
EARLY = 6
FIRST = 5
VMEM_MIB = 52
HALF = 2
F32, BF16 = jnp.float32, jnp.bfloat16


def nt(a, b):
    return lax.dot_general(a, b, (((1,), (1,)), ((), ())), preferred_element_type=F32)


def nn(a, b):
    return lax.dot_general(a, b, (((1,), (0,)), ((), ())), preferred_element_type=F32)


def remote(src, dst, send, recv, **where):
    return pltpu.make_async_remote_copy(
        src_ref=src, dst_ref=dst, send_sem=send, recv_sem=recv,
        device_id=where, device_id_type=pl.DeviceIdType.MESH)


def make_kernel(users, width, quarter, emb, shard_users, n_query):
    w = quarter // J
    piece = quarter // HALF
    rows_blk = 64
    n_rb = users // rows_blk
    lanes = w // 128

    def kern(mask, item, user, queries, fu_out, fit, q_out,
             adj, stage, panel, ps, pk, rs, rx, isum, ut, u0t, usend, urecv, usum,
             rowacc, invu, di, di_sib, di_chip, di_x, di_dg, invi, du, acc, fut, qrow,
             m_sib, ut_sib, du_sib, invu_sib, qacc,
             m_sem, i_sem, in_sem, ps_s, ps_r0, ps_r1, tx_s, tx_r, as_s, as_r, ax_s, ax_r, af_s, af_r,
             u_s, u_r, d_s, d_r, dx_s, dx_r, l_s, l_r, f_s, f_r,
             sm_s, sm_r, su_s, su_r, sd_s, sd_r):
        r = lax.axis_index('row')
        c = lax.axis_index('col')
        sib = r + 1 - 2 * (r % 2)
        xp = (r + 2) % 4
        dg = (sib + 2) % 4
        cols = [(c + k) % 4 for k in (1, 2, 3)]

        def over(n, body, start=0):
            def step(j, carry):
                body(j)
                return carry
            lax.fori_loop(start, n, step, 0)

        def part_of(j):
            return pl.ds(pl.multiple_of(j * w, w), w)

        def piece_of(h):
            return pl.ds(pl.multiple_of(h * piece, piece), piece)

        def mask_copy(b):
            return pltpu.make_async_copy(
                mask.at[:, pl.ds(pl.multiple_of(b * w, w), w)], stage.at[b % NSLOT], m_sem.at[b % NSLOT])

        lead = LEAD * w

        def item_copy(k):
            sl = (pl.ds(0, lead), pl.ds(lead, quarter - lead))[k]
            return pltpu.make_async_copy(item.at[:, sl], panel.at[0, r, :, sl], i_sem.at[k])

        for k in range(2):
            item_copy(k).start()
        user_copy = pltpu.make_async_copy(user, u0t.at[c], in_sem.at[0])
        user_copy.start()
        query_copy = pltpu.make_async_copy(queries, qrow, in_sem.at[1])
        query_copy.start()
        for b in range(3):
            mask_copy(b).start()

        bar = pltpu.get_barrier_semaphore()
        for q in (sib, xp, dg):
            pl.semaphore_signal(bar, inc=1, device_id={'row': q}, device_id_type=pl.DeviceIdType.MESH)
        for q in cols:
            pl.semaphore_signal(bar, inc=1, device_id={'col': q}, device_id_type=pl.DeviceIdType.MESH)
            pl.semaphore_signal(bar, inc=1, device_id={'row': sib, 'col': q}, device_id_type=pl.DeviceIdType.MESH)

        def to_sib(src, dst, send, recv):
            return remote(src, dst, send, recv, row=sib)

        def to_xp(src, dst, send, recv):
            return remote(src, dst, send, recv, row=xp)

        def ps_near(s, j):
            return to_sib(ps.at[0, j], rs.at[s, 0, j], ps_s, ps_r0.at[s % 2])

        def ps_far(s, j):
            return to_sib(ps.at[1, j], rs.at[s, 1, j], ps_s, ps_r1.at[j])

        def ps_near_all(s):
            return to_sib(ps.at[0], rs.at[s, 0], ps_s, ps_r0.at[s % 2])

        def ps_all(s):
            return to_sib(ps, rs.at[s], ps_s, ps_r0.at[s % 2])

        def tx_copy(s, j):
            return to_xp(pk.at[1, j], rx.at[s, j], tx_s, tx_r.at[s % 2, j // 2])

        def tx_pair(s, i):
            two = pl.ds(2 * i, 2)
            return to_xp(pk.at[1, two], rx.at[s, two], tx_s, tx_r.at[s % 2, i])

        def tx_all(s):
            return to_xp(pk.at[1], rx.at[s], tx_s, tx_r.at[s % 2, 0])

        def as_copy(s, sl, q):
            ref = panel.at[s, q, :, sl]
            return to_sib(ref, ref, as_s, as_r)

        def ax_copy(s, sl, q, h):
            ref = panel.at[s, q, :, sl]
            return to_xp(ref, ref, ax_s, ax_r.at[s % 2, h])

        def af_copy(s, sl, q, h):
            ref = panel.at[s, q, :, sl]
            return to_sib(ref, ref, af_s, af_r.at[h])

        whole = pl.ds(0, quarter)

        def share_far(s, j):
            ax_copy(s, part_of(j), r, j // (J // HALF)).start()

        def share_item(s, j):
            as_copy(s, part_of(j), r).start()
            share_far(s, j)

        def user_copies(kind, src, dst, slot):
            return [remote(src, dst.at[slot], u_s, u_r.at[kind], col=q) for q in cols]

        def user_all(kind, buf):
            three = buf.at[pl.ds(0, 3)]
            return remote(three, three, u_s, u_r.at[kind], col=cols[0])

        def dis_copy(q):
            return to_sib(di.at[q], di_sib.at[q], d_s, d_r.at[q])

        def dix_copy(q):
            return to_xp(di_chip.at[q], di_x.at[q], dx_s, dx_r.at[q])

        def chip_degree(q):
            dis_copy(q).wait_recv()
            di_chip[q] = di[q] + di_sib[q]
            dix_copy(q).start()

        rowacc[...] = jnp.zeros_like(rowacc)

        def mask_pass(q, first=0, last=J):
            def mask_step(j):
                b = q * J + j
                mask_copy(b).wait()
                slot = b % NSLOT

                def rows_step(rb, csum):
                    rows = pl.ds(pl.multiple_of(rb * rows_blk, rows_blk), rows_blk)
                    m = stage[slot, rows, :].astype(F32)
                    adj[q, rows, part_of(j)] = m.astype(BF16)
                    part = m[:, :128]
                    for t in range(1, lanes):
                        part = part + m[:, t * 128:(t + 1) * 128]
                    rowacc[rows, :] = rowacc[rows, :] + part
                    for t in range(0, rows_blk, 8):
                        csum = csum + m[t:t + 8, :]
                    return csum

                csum = lax.fori_loop(0, n_rb, rows_step, jnp.zeros((8, w), F32), unroll=8)
                di[q, pl.ds(j, 1), :] = jnp.sum(csum, axis=0, keepdims=True)

                @pl.when(b + NSLOT < 4 * J)
                def _():
                    mask_copy(b + NSLOT).start()

            over(last, mask_step, first)

        for b in range(3, 5):
            mask_copy(b).start()
        with jax.named_scope('mask_0'):
            mask_pass(0, 0, HEAD)
        with jax.named_scope('first_item'):
            item_copy(0).wait()
            for b in range(5, NSLOT):
                mask_copy(b).start()
            pl.semaphore_wait(bar, 9)
            over(LEAD, lambda j: share_far(0, j))
        with jax.named_scope('mask_0b'):
            mask_pass(0, HEAD, NEXT)
            item_copy(1).wait()
            over(EARLY, lambda j: share_far(0, j), LEAD)
            as_copy(0, whole, r).start()
            user_copy.wait()
            query_copy.wait()
            for cp in user_copies(0, u0t.at[c], u0t, c):
                cp.start()
            mask_pass(0, NEXT)
        dis_copy(0).start()
        half = w // 2
        m_copy = to_sib(adj.at[dg, :, pl.ds(0, half)], m_sib, sm_s, sm_r)
        ut_copy = to_sib(ut, ut_sib, su_s, su_r)
        du_all = to_sib(du_sib, du_sib, sd_s, sd_r)
        for q in range(1, 4):
            with jax.named_scope(f'mask_{q}'):
                mask_pass(q, 0, J // 2)
                chip_degree(q - 1)
                if q == 3:
                    m_copy.start()
                    user_all(0, u0t).wait_recv()
                    user_all(0, u0t).wait_send()
                    u0 = jnp.concatenate([u0t[k] for k in range(4)], axis=1)
                    ut[...] = u0
                    ut_copy.start()
                    usum[...] = u0.astype(F32)
                mask_pass(q, J // 2)
            if q < 3:
                dis_copy(q).start()

        with jax.named_scope('degrees'):
            du[c] = nt(jnp.ones((8, 128), BF16), rowacc[...].astype(BF16))[0:1, :]
            for cp in user_copies(4, du.at[c], du, c):
                cp.start()
            for q in cols:
                remote(du.at[c], du_sib.at[c], sd_s, sd_r, row=sib, col=q).start()
            to_sib(du.at[c], du_sib.at[c], sd_s, sd_r).start()
            last_di = [to_sib(di.at[3], di_sib.at[3], l_s, d_r.at[3]), to_xp(di.at[3], di_x.at[3], l_s, dx_r.at[3]),
                       remote(di.at[3], di_dg, l_s, l_r, row=dg)]
            for cp in last_di:
                cp.start()
            over(J, lambda j: share_far(0, j), EARLY)
            with jax.named_scope('wait_di'):
                for q in range(3):
                    dix_copy(q).wait_recv()
                    invi[q] = lax.rsqrt(jnp.maximum(di_chip[q] + di_x[q], 1.0))
                for cp in last_di:
                    cp.wait_recv()
                invi[3] = lax.rsqrt(jnp.maximum((di[3] + di_sib[3]) + (di_x[3] + di_dg[...]), 1.0))
            with jax.named_scope('wait_du'):
                user_all(4, du).wait_recv()
            def spread_degree(d):
                deg = ((d[0] + d[1]) + d[2]) + d[3]
                return jnp.transpose(jnp.broadcast_to(lax.rsqrt(jnp.maximum(deg, 1.0)), (128, users)))

            invu[...] = spread_degree(du)
            du_all.wait_recv()
            invu_sib[...] = spread_degree(du_sib)
            ut_copy.wait()
            m_copy.wait()

        def form(q, j, off=0, n=w):
            def rows_step(rb, carry):
                rows = pl.ds(pl.multiple_of(rb * rows_blk, rows_blk), rows_blk)
                at = pl.ds(pl.multiple_of(j * w + off, n), n)
                m = adj[q, rows, at].astype(F32)
                iu = jnp.concatenate([invu[rows, :]] * (n // 128), axis=1)
                adj[q, rows, at] = ((iu * m) * invi[q, pl.ds(j, 1), off:off + n]).astype(BF16)
                return carry

            lax.fori_loop(0, n_rb, rows_step, 0, unroll=8)

        def form_sib():
            def rows_step(rb, carry):
                rows = pl.ds(pl.multiple_of(rb * rows_blk, rows_blk), rows_blk)
                m = m_sib[rows, :].astype(F32)
                iu = jnp.concatenate([invu_sib[rows, :]] * (half // 128), axis=1)
                m_sib[rows, :] = ((iu * m) * invi[xp, 0:1, 0:half]).astype(BF16)
                return carry

            lax.fori_loop(0, n_rb, rows_step, 0, unroll=8)

        def sum_far(s, j):
            ps_far(s, j).wait_recv()
            pk[1, j] = pk[1, j] + rs[s, 1, j]

        def first_part():
            lo, hi = slice(0, half), slice(half, w)
            form(xp, 0, 0, half)
            form_sib()
            pk[1, 0, :, lo] = nn(ut[...], adj[xp, :, lo]) + nn(ut_sib[...], m_sib[...])
            to_xp(pk.at[1, 0, :, lo], rx.at[0, 0, :, lo], tx_s, tx_r.at[0, 0]).start()
            form(dg, 0, half, half)
            ps[1, 0, :, hi] = nn(ut[...], adj[dg, :, hi])
            hi_copy = to_sib(ps.at[1, 0, :, hi], rs.at[0, 1, 0, :, hi], ps_s, ps_r1.at[0])
            hi_copy.start()
            form(dg, 0, 0, half)
            form(xp, 0, half, half)
            pk[1, 0, :, hi] = nn(ut[...], adj[xp, :, hi])
            form(sib, 0)
            ps[0, 0] = nn(ut[...], adj[sib, :, part_of(0)])
            ps_near(0, 0).start()
            hi_copy.wait_recv()
            pk[1, 0, :, hi] = pk[1, 0, :, hi] + rs[0, 1, 0, :, hi]
            to_xp(pk.at[1, 0, :, hi], rx.at[0, 0, :, hi], tx_s, tx_r.at[0, 0]).start()
            form(r, 0)
            pk[0, 0] = nn(ut[...], adj[r, :, part_of(0)])

        def item_part(s):
            def term(q, j):
                if s == 0:
                    form(q, j)
                return nn(ut[...], adj[q, :, part_of(j)])

            def step(j):
                ps[1, j] = term(dg, j)
                ps_far(s, j).start()
                pk[1, j] = term(xp, j)
                ps[0, j] = term(sib, j)
                ps_near(s, j).start()
                pk[0, j] = term(r, j)
                if s == 0:
                    sum_far(s, j)
                    tx_copy(s, j).start()
                elif s == 1:
                    @pl.when(j > 0)
                    def _():
                        sum_far(s, j - 1)
                        tx_copy(s, j - 1).start()
                else:
                    @pl.when(j > 0)
                    def _():
                        sum_far(s, j - 1)

                    @pl.when((j > 0) & (j <= FIRST))
                    def _():
                        tx_copy(s, j - 1).start()

            if s == 0:
                first_part()
            over(J, step, 0 if s else 1)
            if s:
                sum_far(s, J - 1)
            if s == 1:
                tx_copy(s, J - 1).start()

        def item_finish(s):
            ps_near_all(s).wait_recv()

            def finish(j):
                v = ((pk[0, j] + rs[s, 0, j]) + rx[s, j]).astype(BF16)
                before = panel[0, r, :, part_of(j)].astype(F32) if s == 0 else isum[j]
                total = before + v.astype(F32)
                if s < LAYERS - 1:
                    panel[s + 1, r, :, part_of(j)] = v
                    share_item(s + 1, j)
                    isum[j] = total
                else:
                    fit[j] = (total / (LAYERS + 1)).astype(BF16)

            def step(i):
                tx_pair(s, i).wait_recv()
                finish(2 * i)
                finish(2 * i + 1)

            over(J // 2, step)

        def drain(s):
            as_copy(s, whole, r).wait_send()
            ax_copy(s, whole, r, 0).wait_send()

        def user_part(s):
            def add(q, h):
                acc[...] = acc[...] + nt(adj[q, :, piece_of(h)], panel[s, q, :, piece_of(h)])

            acc[...] = jnp.zeros_like(acc)
            over(HALF, lambda h: add(r, h))
            as_copy(s, whole, sib).wait_recv()
            over(HALF, lambda h: add(sib, h))

            def far(h):
                ax_copy(s, piece_of(h), xp, h).wait_recv()
                af_copy(s, piece_of(h), xp, h).start()
                add(xp, h)
                af_copy(s, piece_of(h), dg, h).wait_recv()
                add(dg, h)

            over(HALF, far)
            if s == 0:
                user_all(4, du).wait_send()
            t = jnp.transpose(acc[...])
            usend[s] = t
            urecv[s, c] = t
            for cp in user_copies(s + 1, usend.at[s], urecv.at[s], c):
                cp.start()

        def user_finish(s):
            user_all(s + 1, urecv.at[s]).wait_recv()
            user_all(s + 1, urecv.at[s]).wait_send()
            v = (((urecv[s, 0] + urecv[s, 1]) + urecv[s, 2]) + urecv[s, 3]).astype(BF16)
            ut[...] = v
            usum[...] = usum[...] + v.astype(F32)

        for s in range(LAYERS):
            with jax.named_scope(f'item_part_{s}'):
                item_part(s)
            with jax.named_scope(f'user_part_{s}'):
                user_part(s)
                drain(s)
            if s < LAYERS - 1:
                with jax.named_scope(f'item_finish_{s}'):
                    item_finish(s)
                    tx_all(s).wait_send()
            with jax.named_scope(f'user_finish_{s}'):
                if s == 0:
                    to_sib(ps.at[0], rs.at[0, 0], ps_s, ps_r0.at[0]).wait_send()
                    to_sib(ps.at[1, pl.ds(1, J - 1)], rs.at[0, 1, pl.ds(1, J - 1)], ps_s, ps_r0.at[0]).wait_send()
                    to_sib(ps.at[1, 0, :, pl.ds(half, half)], rs.at[0, 1, 0, :, pl.ds(half, half)], ps_s, ps_r0.at[0]).wait_send()
                else:
                    ps_all(s).wait_send()
                af_copy(s, whole, xp, 0).wait_send()
                user_finish(s)

        with jax.named_scope('final_users'):
            fu = (usum[...] / (LAYERS + 1)).astype(BF16)
            for k in range(4):
                fut[r, k] = fu[:, k * shard_users:(k + 1) * shard_users]
            fu_out[...] = fut[r, c]
            cross = to_xp(fut.at[r, c], fut.at[r, c], f_s, f_r.at[0])
            cross.start()
            over(J - 1, lambda j: tx_copy(2, j).start(), FIRST)

            @pl.when(r % 2 == 0)
            def _():
                tx_copy(2, J - 1).start()
            own = to_sib(fut.at[r], fut.at[r], f_s, f_r.at[1])
            own.start()
            cross.wait_recv()
            spread = [remote(fut.at[xp, c], fut.at[xp, c], f_s, f_r.at[2], col=q) for q in cols]
            for cp in spread:
                cp.start()
            three = fut.at[xp, pl.ds(0, 3)]
            spread_all = remote(three, three, f_s, f_r.at[2], col=cols[0])
            spread_all.wait_recv()
            other = to_sib(fut.at[xp], fut.at[xp], f_s, f_r.at[3])
            other.start()
            own.wait_recv()

            def pick(q):
                ids = lax.broadcasted_iota(jnp.int32, (users, n_query), 0) + q * users
                onehot = jnp.where(ids == qrow[...], 1.0, 0.0).astype(BF16)
                return nn(jnp.concatenate([fut[q, k] for k in range(4)], axis=1), onehot)

            qacc[...] = (pick(r) + pick(sib)) + pick(xp)

            other.wait_recv()
            @pl.when(r % 2 == 1)
            def _():
                tx_copy(2, J - 1).start()

            q_out[...] = jnp.transpose(qacc[...] + pick(dg)).astype(BF16)

            three = pl.ds(0, 3)
            to_sib(di.at[three], di_sib.at[three], d_s, d_r.at[0]).wait_send()
            to_xp(di_chip.at[three], di_x.at[three], dx_s, dx_r.at[0]).wait_send()
            to_sib(di.at[three], di_sib.at[three], l_s, d_r.at[0]).wait_send()
            du_all.wait_send()
            to_sib(fut.at[three], fut.at[three], f_s, f_r.at[0]).wait_send()
        with jax.named_scope('item_finish_2'):
            item_finish(2)
        with jax.named_scope('end'):
            tx_all(2).wait_send()

    dma = pltpu.SemaphoreType.DMA
    scratch = [
        pltpu.VMEM((4, users, quarter), BF16),
        pltpu.VMEM((NSLOT, users, w), jnp.int32),
        pltpu.VMEM((3, 4, emb, quarter), BF16),
        pltpu.VMEM((2, J, emb, w), F32),
        pltpu.VMEM((2, J, emb, w), F32),
        pltpu.VMEM((3, 2, J, emb, w), F32),
        pltpu.VMEM((3, J, emb, w), F32),
        pltpu.VMEM((J, emb, w), F32),
        pltpu.VMEM((emb, users), BF16),
        pltpu.VMEM((4, emb, shard_users), BF16),
        pltpu.VMEM((3, emb, users), F32),
        pltpu.VMEM((3, 4, emb, users), F32),
        pltpu.VMEM((emb, users), F32),
        pltpu.VMEM((users, 128), F32),
        pltpu.VMEM((users, 128), F32),
        pltpu.VMEM((4, J, w), F32),
        pltpu.VMEM((4, J, w), F32),
        pltpu.VMEM((4, J, w), F32),
        pltpu.VMEM((4, J, w), F32),
        pltpu.VMEM((J, w), F32),
        pltpu.VMEM((4, J, w), F32),
        pltpu.VMEM((4, 1, users), F32),
        pltpu.VMEM((users, emb), F32),
        pltpu.VMEM((4, 4, emb, shard_users), BF16),
        pltpu.VMEM((1, n_query), jnp.int32),
        pltpu.VMEM((users, w // 2), BF16),
        pltpu.VMEM((emb, users), BF16),
        pltpu.VMEM((4, 1, users), F32),
        pltpu.VMEM((users, 128), F32),
        pltpu.VMEM((emb, n_query), F32),
        dma((NSLOT,)), dma((2,)), dma((2,)),
        dma, dma((2,)), dma((J,)),
        dma, dma((2, J // 2)),
        dma, dma,
        dma, dma((2, HALF)),
        dma, dma((HALF,)),
        dma, dma((5,)),
        dma, dma((4,)), dma, dma((4,)), dma, dma,
        dma, dma((4,)),
        dma, dma, dma, dma, dma, dma,
    ]
    vm, hbm = pl.BlockSpec(memory_space=pltpu.VMEM), pl.BlockSpec(memory_space=pltpu.HBM)
    return pl.pallas_call(
        kern,
        out_shape=(jax.ShapeDtypeStruct((emb, shard_users), BF16),
                   jax.ShapeDtypeStruct((J, emb, w), BF16),
                   jax.ShapeDtypeStruct((n_query, emb), BF16)),
        in_specs=[hbm, hbm, hbm, hbm],
        out_specs=(vm, vm, vm),
        scratch_shapes=scratch,
        name='propagate',
        compiler_params=pltpu.CompilerParams(
            collective_id=0, has_side_effects=True, vmem_limit_bytes=VMEM_MIB * 2 ** 20))


def score_kernel(query, fit, fu, scores, item_out, user_out, buf, s_sem, i_sem, u_sem):
    n, _, w = fit.shape
    user_copy = pltpu.make_async_copy(fu, user_out, u_sem)
    user_copy.start()

    def cols(j):
        return pl.ds(pl.multiple_of(j * w, w), w)

    def step(j, carry):
        buf[:, cols(j)] = nn(query[...], fit[j])
        rows = buf.shape[0] // 2
        for k in range(2):
            part = (pl.ds(k * rows, rows), cols(j))
            pltpu.make_async_copy(buf.at[part], scores.at[part], s_sem).start()
        pltpu.make_async_copy(fit.at[j], item_out.at[:, cols(j)], i_sem).start()
        return carry

    lax.fori_loop(0, n, step, 0)
    pltpu.make_async_copy(buf, scores, s_sem).wait()
    pltpu.make_async_copy(item_out, item_out, i_sem).wait()
    user_copy.wait()


def score(query, fit, fu):
    n_query, emb = query.shape
    n, _, w = fit.shape
    vm, hbm = pl.BlockSpec(memory_space=pltpu.VMEM), pl.BlockSpec(memory_space=pl.ANY)
    return pl.pallas_call(
        score_kernel,
        out_shape=(jax.ShapeDtypeStruct((n_query, n * w), F32), jax.ShapeDtypeStruct((emb, n * w), BF16),
                   jax.ShapeDtypeStruct(fu.shape, BF16)),
        in_specs=[vm, vm, vm],
        out_specs=(hbm, hbm, hbm),
        scratch_shapes=[pltpu.VMEM((n_query, n * w), F32)] + [pltpu.SemaphoreType.DMA] * 3,
        name='score',
        compiler_params=pltpu.CompilerParams(vmem_limit_bytes=12 * 2 ** 20),
    )(query, fit, fu)


def solution(mesh):
    def device_step(mask_blk, user_shard, item_shard, queries):
        users, width = mask_blk.shape
        quarter, emb = item_shard.shape
        n_query = queries.shape[0]
        call = make_kernel(users, width, quarter, emb, user_shard.shape[0], n_query)
        fu, fit, query = call(*[pltpu.with_memory_space_constraint(a, pltpu.HBM) for a in (
            mask_blk, item_shard.T, user_shard.T, queries.reshape(1, n_query))])
        scores, final_item, final_user = score(query, fit, fu)
        return final_user.T, final_item.T, scores

    return jax.shard_map(device_step, mesh=mesh, in_specs=(P('row', 'col'), P(('row', 'col'), None), P(('col', 'row'), None), P()), out_specs=(P(('row', 'col'), None), P(('col', 'row'), None), P(None, ('col', 'row'))), check_vma=False)
```
